32 devices in a mesh: clip: 2 (over y), tm: 4 (over z), space: 2 (over x), chan: 2 (over core).
Axes of the slice: x: 2, y: 2, z: 4, core: 2. Of those that a mesh axis runs over, the one named last changes fastest.
Arguments:
- features: bfloat16 [16, 8, 90, 256], P(('clip', 'tm'), 'space'), parts along dimension 0, may hold values from -700 to 700
- hidden: bfloat16 [16, 8, 90, 256], P(('clip', 'tm'), 'space'), parts along dimension 0, may hold values from -700 to 700
- cotangent: bfloat16 [16, 8, 90, 256], P(('clip', 'tm'), 'space'), parts along dimension 0, may hold values from -6 to 6
- kernel_one: bfloat16 [256, 3, 3, 3, 256], P(None, None, None, None, 'chan'), may hold values from -0.078125 to 0.078125
- kernel_two: bfloat16 [256, 3, 3, 3, 256], P(None, None, None, None, 'chan'), may hold values from -0.078125 to 0.078125
- gains: float32 [2, 256], replicated, may hold values from 0.25 to 1.75
Outputs:
- feature_grad: bfloat16 [16, 8, 90, 256], P(('clip', 'tm'), 'space', None, 'chan'), parts along dimension 0
- delta_one: float32 [512, 3, 3, 3, 256], P(('clip', 'tm', 'space'), None, None, None, 'chan'), parts along dimension 0
- delta_two: float32 [512, 3, 3, 3, 256], P(('clip', 'tm', 'space'), None, None, None, 'chan'), parts along dimension 0
- gain_grads: float32 [4, 256], P('clip', 'chan'), parts along dimension 0
The draws below stay inside these ranges and needn't reach their ends.
There are 2 independent parts, one for each index of `clip`. The reference program is written for one: setup_inputs(seed, part) draws one part's arguments, and reference() takes and returns one part's arrays. A program takes and returns all parts, laid end to end along the dimension named above; an argument that names none is the same for every part. Nothing has to cross between parts.
All inputs are finite; a program needn't handle non-finite values.
Results may differ from the reference program's by a relative error of at most 0.005.
Values may be sent and summed in bfloat16 or wider, within the bound.
A program may use at most 128 MiB of HBM per device.

```python
import math
import jax
import jax.numpy as jnp
from jax import lax

C = 256
GROUPS = 32
W = 90
FRAMES = 8
HEIGHT = 8


def field_draw(key):
    key_base, key_rows, key_chan = jax.random.split(key, 3)
    shape = (FRAMES, HEIGHT, W, C)
    row_scale = 0.2 * jnp.exp(jax.random.uniform(key_rows, (FRAMES, HEIGHT, 1, 1), jnp.float32, 0.0, math.log(10.0)))
    chan_scale = jnp.exp(jax.random.uniform(key_chan, (1, 1, 1, C), jnp.float32, 0.0, math.log(4.0)))
    position = jnp.arange(FRAMES, dtype=jnp.float32).reshape(FRAMES, 1, 1, 1) / max(FRAMES - 1, 1)
    base = jnp.clip(jax.random.normal(key_base, shape, jnp.float32), -4.0, 4.0)
    rise = jnp.exp(0.5 * math.log(3.0) * position)
    return base * row_scale * chan_scale * rise


def draw_features(key, part):
    return field_draw(jax.random.fold_in(key, 11)).astype(jnp.bfloat16)


def draw_hidden(key, part):
    return field_draw(jax.random.fold_in(key, 23)).astype(jnp.bfloat16)


def block_levels(rng, shape, cuts, least, high):
    loudness, own = 1.0, jax.random.fold_in(rng, 6)
    for dim, blocks in cuts:
        heights = jnp.exp(jax.random.uniform(jax.random.fold_in(own, dim), (blocks,), jnp.float32, least / len(cuts), high / len(cuts)))
        loudness = loudness * jnp.repeat(heights, shape[dim] // blocks).reshape([-1 if axis == dim else 1 for axis in range(len(shape))])
    return loudness


def scatter_about(stream_key, extent, deviation, bound, cuts=(), kind=jnp.bfloat16):
    entries = deviation * jax.random.normal(stream_key, extent, jnp.float32)
    if cuts:
        entries = entries * block_levels(stream_key, extent, cuts, -0.22, 0.18)
    return jnp.clip(entries, -bound, bound).astype(kind)


def setup_inputs(seed: int = 0, part: int = 0) -> dict:
    streams_of = jax.random.split(jax.random.key(seed), 7)
    part_splits = jax.random.split(jax.random.fold_in(streams_of[6], part), 7)
    features = draw_features(jax.random.fold_in(jax.random.fold_in(streams_of[6], part), 71), part)
    hidden = draw_hidden(jax.random.fold_in(jax.random.fold_in(streams_of[6], part), 71), part)
    cotangent = scatter_about(part_splits[2], (FRAMES, HEIGHT, W, C), 1.0, 6.0, ((0, 4), (1, 2)))
    kernel_one = scatter_about(streams_of[3], (C, 3, 3, 3, C), (27 * C) ** -0.5, 0.078125, ((4, 2),))
    kernel_two = scatter_about(streams_of[4], (C, 3, 3, 3, C), (27 * C) ** -0.5, 0.078125, ((4, 2),))
    gains = jnp.clip(1.0 + 0.15 * jax.random.normal(streams_of[5], (2, C), jnp.float32), 0.25, 1.75)
    return dict(features=features, hidden=hidden, cotangent=cotangent, kernel_one=kernel_one, kernel_two=kernel_two, gains=gains)


epsilon = 1e-06

def moments(field, gain, members):
    per = field.shape[3] // GROUPS
    total = lax.optimization_barrier(jnp.sum(field, axis=(0, 1, 2))).reshape(GROUPS, per)
    square = lax.optimization_barrier(jnp.sum(field * field, axis=(0, 1, 2))).reshape(GROUPS, per)
    mean = lax.optimization_barrier(jnp.sum(total, axis=1)) / members
    spread = lax.optimization_barrier(jnp.sum(square, axis=1)) / members - mean * mean
    scale = jnp.repeat(lax.rsqrt(spread + epsilon), per)
    centred = (field - jnp.repeat(mean, per)) * scale
    return (centred, centred * gain, scale)

def norm_back(upstream, centred, scaled, gain, scale, members):
    per = upstream.shape[3] // GROUPS
    gate = jax.nn.sigmoid(scaled)
    slope = upstream * gate * (1.0 + scaled * (1.0 - gate))
    plain = lax.optimization_barrier(jnp.sum(slope, axis=(0, 1, 2)))
    weighted = lax.optimization_barrier(jnp.sum(slope * centred, axis=(0, 1, 2)))
    first = jnp.repeat(lax.optimization_barrier(jnp.sum((gain * plain).reshape(-1, per), axis=1)), per) / members
    second = jnp.repeat(lax.optimization_barrier(jnp.sum((gain * weighted).reshape(-1, per), axis=1)), per) / members
    return (scale * (slope * gain - first - centred * second), weighted)

def conv_back(active, grad, kernel):
    frames, height, width, channels = active.shape
    padded = jnp.pad(grad.astype(jnp.float32), ((0, 2), (1, 1), (1, 1), (0, 0)))
    flipped = jnp.flip(jnp.transpose(kernel.astype(jnp.float32), (1, 2, 3, 4, 0)), (0, 1, 2))
    back = lax.conv_general_dilated(padded[None], flipped, (1, 1, 1), ((0, 0), (0, 0), (0, 0)), dimension_numbers=('NDHWC', 'DHWIO', 'NDHWC'), precision=lax.Precision.HIGHEST)[0]
    flat = active.reshape(-1, channels).astype(jnp.float32)
    pieces = []
    for frame_tap in range(3):
        for row_tap in range(3):
            for col_tap in range(3):
                window = padded[2 - frame_tap:2 - frame_tap + frames, 2 - row_tap:2 - row_tap + height, 2 - col_tap:2 - col_tap + width].reshape(-1, channels)
                pieces.append(lax.dot_general(flat, window, (((0,), (0,)), ((), ())), precision=lax.Precision.HIGHEST))
    delta = jnp.stack(pieces, axis=1).reshape(channels, 3, 3, 3, channels)
    return (delta, back)

def reference(features, hidden, cotangent, kernel_one, kernel_two, gains):
    members = float(FRAMES * HEIGHT * W * (C // GROUPS))
    centred_one, scaled_one, scale_one = moments(features.astype(jnp.float32), gains[0], members)
    centred_two, scaled_two, scale_two = moments(hidden.astype(jnp.float32), gains[1], members)
    active_one = (scaled_one * jax.nn.sigmoid(scaled_one)).astype(jnp.bfloat16)
    active_two = (scaled_two * jax.nn.sigmoid(scaled_two)).astype(jnp.bfloat16)
    delta_two, back_two = conv_back(active_two, cotangent, kernel_two)
    grad_two, weighted_two = norm_back(back_two, centred_two, scaled_two, gains[1], scale_two, members)
    grad_hidden = grad_two.astype(jnp.bfloat16)
    delta_one, back_one = conv_back(active_one, grad_hidden, kernel_one)
    grad_one, weighted_one = norm_back(back_one, centred_one, scaled_one, gains[0], scale_one, members)
    feature_grad = (cotangent.astype(jnp.float32) + grad_one).astype(jnp.bfloat16)
    return (feature_grad, delta_one, delta_two, jnp.stack([weighted_one, weighted_two]))
```

```python
import functools

import jax
import jax.numpy as jnp
from jax import lax
from jax.experimental import pallas as pl
from jax.experimental.pallas import tpu as pltpu
from jax.sharding import PartitionSpec as P

GROUPS = 32
EPS = 1e-06
MESH = pl.DeviceIdType.MESH
F32 = jnp.float32
BF16 = jnp.bfloat16


def group_sums(values, per):
    channels = values.shape[1]
    row = lax.broadcasted_iota(jnp.int32, (channels, channels), 0) // per
    col = lax.broadcasted_iota(jnp.int32, (channels, channels), 1) // per
    same = jnp.where(row == col, 1.0, 0.0).astype(F32)
    return jnp.dot(values, same, precision=lax.Precision.HIGHEST, preferred_element_type=F32)


def body(
    sizes,
    f_ref, h_ref, cot_ref, k1_ref, k2_ref, gain_ref,
    fg_ref, d1_ref, d2_ref, w_ref,
    grads, taps, gh, kcat, turned, raw, act, acc, xs, xr, vec, r0, r2, r1, out, got, perm,
    k_sem, gx_s, gx_r, gz_s, gz_r, ge_s, ge_r, gr_s, gr_r, gg_s, gg_r,
    ai_s, ai_r, an_s, an_r, ad_s, ad_r, dl_s, dl_r, xsem_s, xsem_r, ar_s, ar_r,
):
    width, n_t, n_s, q = sizes
    frames, height, padded, channels = cot_ref.shape
    half = channels // 2
    per = channels // GROUPS
    n = n_t * n_s
    nj = n_t // q
    rows = frames * height * padded
    lanes = height * padded
    tall = n_s * height
    share = channels // n
    cs = channels // (q * n_s)
    hc = cs // 2
    t = lax.axis_index("tm")
    s = lax.axis_index("space")
    chan = lax.axis_index("chan")
    partner = 1 - chan
    rank = t * n_s + s
    r = lax.rem(t, q)
    p = t // q
    members = float(frames * height * width * per * n)
    mine = pl.ds(pl.multiple_of(chan * half, half), half)
    theirs = pl.ds(pl.multiple_of(partner * half, half), half)
    own_rows = pl.ds(s * height, height)
    own_frames = pl.ds(r * frames, frames)
    next_frames = pl.ds((r + 1) * frames, frames)
    sibling = {"chan": partner}

    def place(j):
        return {"tm": j // n_s, "space": lax.rem(j, n_s)}

    def peer(k):
        return lax.rem(rank + k, n)

    def each_peer(fn):
        def step(k, carry):
            fn(k)
            return carry

        lax.fori_loop(1, n, step, 0)

    def remote(src, dst, send, recv, device):
        return pltpu.make_async_remote_copy(
            src_ref=src, dst_ref=dst, send_sem=send, recv_sem=recv,
            device_id=device, device_id_type=MESH,
        )

    def kernel_copy(layer, source, c):
        return pltpu.make_async_copy(
            source.at[:, c], kcat.at[layer, :, :, c * half : (c + 1) * half], k_sem.at[layer, c]
        )

    for c in range(3):
        kernel_copy(0, k2_ref, c).start()
    for c in range(3):
        kernel_copy(1, k1_ref, c).start()

    barrier = pltpu.get_barrier_semaphore()
    pl.semaphore_signal(barrier, inc=1, device_id=sibling, device_id_type=MESH)
    each_peer(
        lambda k: pl.semaphore_signal(barrier, inc=1, device_id=place(peer(k)), device_id_type=MESH)
    )
    for layer in range(2):
        edge = jnp.zeros((q * frames + 2, 1, padded, 3 * half), BF16)
        taps[layer, :, 0:1] = edge
        taps[layer, :, tall + 1 : tall + 2] = edge

        @pl.when(t == n_t - 1)
        def _(layer=layer):
            def clear(f, carry):
                taps[layer, q * frames + f] = jnp.zeros((tall + 2, padded, 3 * half), BF16)
                return carry

            lax.fori_loop(0, 2, clear, 0)

    pl.semaphore_wait(barrier, n)

    def inside(value, count):
        return (value >= 0) & (value < count)

    def moves(layer, source):
        box = grads.at[layer]
        found = []
        before = jnp.where(r > 0, r, q) * frames
        sent = pl.ds(before, frames)

        def add(kind, go, src, dst, to, come, land, sender, send, recv):
            found.append((
                kind, go, lambda: remote(src, dst, send, recv, to),
                come, lambda: remote(land, land, send, recv, sender),
            ))

        for d, (ds, row) in enumerate(((1, height - 1), (-1, 0))):
            back = (s - ds) * height + row
            add(
                "near",
                (t > 0) & inside(s + ds, n_s),
                source.at[:, row : row + 1],
                box.at[sent, pl.ds(s * height + row, 1)],
                {"tm": t - 1, "space": s + ds},
                (t + 1 < n_t) & inside(s - ds, n_s),
                box.at[next_frames, pl.ds(back, 1)],
                {"tm": t + 1, "space": s - ds},
                ge_s.at[layer, d], ge_r.at[layer, d],
            )
        add(
            "near", t > 0, source, box.at[sent, own_rows], {"tm": t - 1},
            t + 1 < n_t, box.at[next_frames, own_rows], {"tm": t + 1},
            gz_s.at[layer], gz_r.at[layer],
        )
        for k in range(1, n_s):
            to, back = lax.rem(s + k, n_s), lax.rem(s + n_s - k, n_s)
            add(
                "near", None, source, box.at[own_frames, own_rows], {"space": to},
                None, box.at[own_frames, pl.ds(back * height, height)], {"space": back},
                gx_s.at[layer, k], gx_r.at[layer, k],
            )
        if q > 1:
            for k in sorted(range(1 - n_s, n_s), key=abs):
                i = k + n_s - 1
                earlier = pl.ds((r - 1) * frames, frames)
                add(
                    "side" if k == 0 else "far",
                    (r < q - 1) & inside(s + k, n_s),
                    source,
                    box.at[own_frames, own_rows],
                    {"tm": t + 1, "space": s + k},
                    (r > 0) & inside(s - k, n_s),
                    box.at[earlier, pl.ds((s - k) * height, height)],
                    {"tm": t - 1, "space": s - k},
                    gg_s.at[layer, i], gg_r.at[layer, i],
                )
                if k == 0:
                    continue
                low, count = (0, height) if abs(k) > 1 else ((0, height - 1) if k > 0 else (1, height - 1))
                add(
                    "far",
                    (r > 0) & inside(s + k, n_s),
                    source.at[:, low : low + count],
                    box.at[own_frames, pl.ds(s * height + low, count)],
                    {"tm": t - 1, "space": s + k},
                    (r < q - 1) & inside(s - k, n_s),
                    box.at[next_frames, pl.ds((s - k) * height + low, count)],
                    {"tm": t + 1, "space": s - k},
                    gr_s.at[layer, i], gr_r.at[layer, i],
                )
        return found

    def when(predicate, action):
        if predicate is None:
            action()
        else:
            pl.when(predicate)(action)

    def send_moves(found, kinds):
        for kind, go, copy, _, _ in found:
            if kind in kinds:
                when(go, lambda copy=copy: copy().start())

    def take_moves(found, kinds):
        for kind, _, _, come, copy in found:
            if kind in kinds:
                when(come, lambda copy=copy: copy().wait_recv())

    def end_moves(found):
        for _, go, copy, _, _ in found:
            when(go, lambda copy=copy: copy().wait_send())

    def set_rows(to_r, to_s):
        start = (to_r * n_s + to_s) * cs + chan * hc
        return pl.ds(pl.multiple_of(start, hc), hc)

    my_half = pl.ds(pl.multiple_of(chan * hc, hc), hc)

    def strip(at):
        return pl.ds(pl.multiple_of(at * lanes, lanes), lanes)

    def field_moves(layer):
        found = []
        for dr in range(q):
            for k in range(n_s):
                if dr == 0 and k == 0:
                    continue
                to_r, to_s = lax.rem(r + dr, q), lax.rem(s + k, n_s)
                from_r, from_s = lax.rem(r + q - dr, q), lax.rem(s + n_s - k, n_s)
                src = turned.at[layer, :, set_rows(to_r, to_s)]
                dst = raw.at[layer, pl.ds(2 + r * frames, frames), my_half, strip(s)]
                land = raw.at[layer, pl.ds(2 + from_r * frames, frames), my_half, strip(from_s)]
                sems = (ai_s.at[layer, dr, k], ai_r.at[layer, dr, k])
                found.append((
                    "in", None,
                    functools.partial(remote, src, dst, *sems, {"tm": p * q + to_r, "space": to_s}),
                    None,
                    functools.partial(remote, land, land, *sems, {"tm": p * q + from_r, "space": from_s}),
                ))
        for to_r in range(q):
            for k in range(n_s):
                to_s, from_s = lax.rem(s + k, n_s), lax.rem(s + n_s - k, n_s)
                src = turned.at[layer, frames - 2 : frames, set_rows(to_r, to_s)]
                dst = raw.at[layer, 0:2, my_half, strip(s)]
                land = raw.at[layer, 0:2, my_half, strip(from_s)]
                sems = (an_s.at[layer, to_r, k], an_r.at[layer, k])
                found.append((
                    "on", (r == q - 1) & (p + 1 < nj),
                    functools.partial(remote, src, dst, *sems, {"tm": (p + 1) * q + to_r, "space": to_s}),
                    (p > 0) if to_r == 0 else False,
                    functools.partial(remote, land, land, *sems, {"tm": p * q - 1, "space": from_s}),
                ))
        return found

    def take_fields(found):
        for _, _, _, come, copy in found:
            if come is not False:
                when(come, lambda copy=copy: copy().wait_recv())

    def across(layer):
        half_set = raw.at[layer, :, my_half]
        return remote(half_set, half_set, ad_s.at[layer], ad_r.at[layer], sibling)

    def across_land(layer):
        other = raw.at[layer, :, pl.ds(pl.multiple_of(partner * hc, hc), hc)]
        return remote(other, other, ad_s.at[layer], ad_r.at[layer], sibling)

    def sums_copy(layer, buf, k, slot):
        return remote(
            buf.at[slot], buf.at[slot], ar_s.at[layer, k], ar_r.at[layer, slot], place(peer(k))
        )

    def sums_start(layer, buf, values):
        buf[rank] = values
        each_peer(lambda k: sums_copy(layer, buf, k, rank).start())

    def sums_finish(layer, buf):
        each_peer(lambda k: sums_copy(layer, buf, k, peer(k)).wait_recv())
        return jnp.sum(buf[...], axis=0)

    def sums_end(layer, buf):
        each_peer(lambda k: sums_copy(layer, buf, k, rank).wait_send())

    def block_copy(layer, k, b):
        to = lax.rem(p + k, nj)
        return remote(
            out.at[layer, to, b], got.at[layer, k, b], dl_s.at[layer, k, b], dl_r.at[layer, k, b],
            {"tm": to * q + r},
        )

    def cross(layer):
        return remote(xs.at[layer], xr.at[layer], xsem_s.at[layer], xsem_r.at[layer], sibling)

    column = lax.rem(lax.broadcasted_iota(jnp.int32, (rows, 1), 0), padded)
    real = column < width

    def fill(layer, f, row, count):
        cells = grads[layer, f, pl.ds(row, count)].reshape(count * padded, half).astype(F32)
        size = count * padded
        ahead = pltpu.roll(cells, size - 1, 0)
        behind = pltpu.roll(cells, 1, 0)
        for c, value in enumerate((ahead, cells, behind)):
            taps[layer, f, pl.ds(row + 1, count), :, c * half : (c + 1) * half] = value.astype(
                BF16
            ).reshape(count, padded, half)

    def fill_frames(layer, first, strips):
        def step(i, carry):
            f, at = i // len(strips), lax.rem(i, len(strips))
            fill(layer, first + f, strips[0] * height if len(strips) == 1 else at * height, height)
            return carry

        lax.fori_loop(0, frames * len(strips), step, 0)

    def fill_near(layer):
        fill_frames(layer, r * frames, list(range(n_s)))

        @pl.when(t + 1 < n_t)
        def _():
            for f in range(frames):
                fill(layer, (r + 1) * frames + f, s * height, height)

        for row, ok in ((s * height - 1, s > 0), ((s + 1) * height, s + 1 < n_s)):
            @pl.when(ok & (t + 1 < n_t))
            def _(row=row):
                for f in range(frames):
                    fill(layer, (r + 1) * frames + f, row, 1)

    def fill_far(layer):
        for other in range(q):
            @pl.when(r != other)
            def _(other=other):
                fill_frames(layer, other * frames, list(range(n_s)))

    def conv(layer, source):
        for c in range(3):
            kernel_copy(layer, source, c).wait()
        for f in range(frames):
            total = None
            for ab in range(9):
                a, b = ab // 3, ab % 3
                left = taps[
                    layer, r * frames + (2 - a + f), pl.ds(s * height + (2 - b), height)
                ].reshape(lanes, 3 * half)
                term = lax.dot_general(
                    left, kcat[layer, ab], (((1,), (1,)), ((), ())), preferred_element_type=F32
                )
                total = term if total is None else total + term
            acc[f * lanes : (f + 1) * lanes] = total
        xs[layer] = acc[:, theirs].astype(BF16)
        cross(layer).start()

    def norm_back(field_ref, base, layer):
        cross(layer).wait_recv()
        upstream = acc[:, mine] + xr[layer].astype(F32)
        field = field_ref[:, :, :, mine].reshape(rows, half).astype(F32)
        scale = vec[base + 1 : base + 2, mine]
        gain = vec[base + 2 : base + 3, mine]
        centred = (field - vec[base : base + 1, mine]) * scale
        scaled = centred * gain
        gate = jax.nn.sigmoid(scaled)
        slope = jnp.where(real, upstream * gate * (1.0 + scaled * (1.0 - gate)), 0.0)
        acc[:, mine] = slope
        parts = [
            jnp.sum(slope, axis=0, keepdims=True),
            jnp.sum(slope * centred, axis=0, keepdims=True),
            jnp.zeros((6, half), F32),
        ]
        sums_start(layer + 1, (r2, r1)[layer], jnp.concatenate(parts, axis=0))

    def norm_end(field_ref, base, layer, w_row):
        totals = sums_finish(layer + 1, (r2, r1)[layer])
        w_ref[w_row : w_row + 1] = totals[1:2]
        scale = vec[base + 1 : base + 2, mine]
        gain = vec[base + 2 : base + 3, mine]
        means = group_sums(totals * gain, per) / members
        field = field_ref[:, :, :, mine].reshape(rows, half).astype(F32)
        centred = (field - vec[base : base + 1, mine]) * scale
        grad = scale * (acc[:, mine] * gain - means[0:1] - centred * means[1:2])
        return jnp.where(real, grad, 0.0)

    def turn(field_ref, layer):
        for f in range(frames):
            cells = field_ref[f].reshape(lanes, channels)
            flat = lax.dot_general(
                perm[...], cells, (((1,), (1,)), ((), ())), preferred_element_type=F32
            ).astype(BF16)
            turned[layer, f] = flat
        raw[layer, pl.ds(2 + r * frames, frames), my_half, strip(s)] = turned[layer, :, set_rows(r, s)]

    def activate(layer, base):
        pick = perm[pl.ds(pl.multiple_of((r * n_s + s) * cs, cs), cs)].astype(F32)
        cols = lax.dot_general(
            pick, vec[...], (((1,), (1,)), ((), ())),
            precision=lax.Precision.HIGHEST, preferred_element_type=F32,
        )
        mean, scale, gain = (cols[:, base + i : base + i + 1] for i in range(3))
        spot = lax.rem(lax.broadcasted_iota(jnp.int32, (1, tall * padded), 1), padded)

        def step(f, carry):
            field = raw[layer, f].astype(F32)
            scaled = (field - mean) * scale * gain
            keep = (spot < width) & ((f >= 2) | (p > 0))
            active = jnp.where(keep, scaled * jax.nn.sigmoid(scaled), 0.0)
            act[layer, f] = active.astype(BF16)
            return carry

        lax.fori_loop(0, q * frames + 2, step, 0)

    def delta(layer, own):
        for b in range(3):
            product = None
            for f in range(q * frames):
                left = act[layer, f : f + 3].reshape(3 * cs, tall * padded)
                right = taps[layer, f, 2 - b : 2 - b + tall].reshape(tall * padded, 3 * half)
                term = jnp.dot(left, right, preferred_element_type=F32)
                product = term if product is None else product + term
            small = product.astype(BF16)
            for j in range(nj):
                for a in range(3):
                    low = a * cs + j * share
                    out[layer, j, b, a] = small[low : low + share]

                @pl.when(p == j)
                def _(j=j):
                    for a in range(3):
                        low = a * cs + j * share
                        for c in range(3):
                            own[a * 9 + b * 3 + c] = product[
                                low : low + share, c * half : (c + 1) * half
                            ]

            for k in range(1, nj):
                block_copy(layer, k, b).start()

    moves_two = moves(0, cot_ref.at[:, :, :, mine])
    moves_one = moves(1, gh)
    send_moves(moves_two, ("near", "side"))
    grads[0, own_frames, own_rows] = cot_ref[:, :, :, mine]

    field_one = f_ref[...].reshape(rows, channels).astype(F32)
    field_two = h_ref[...].reshape(rows, channels).astype(F32)
    parts = [
        jnp.sum(field_one, axis=0, keepdims=True),
        jnp.sum(field_one * field_one, axis=0, keepdims=True),
        jnp.sum(field_two, axis=0, keepdims=True),
        jnp.sum(field_two * field_two, axis=0, keepdims=True),
        jnp.zeros((4, channels), F32),
    ]
    sums_start(0, r0, jnp.concatenate(parts, axis=0))

    place_row = lax.broadcasted_iota(jnp.int32, (channels, channels), 0)
    place_col = lax.broadcasted_iota(jnp.int32, (channels, channels), 1)
    element = lax.rem(place_row, share)
    block = lax.rem(place_row // share, nj)
    which = place_row // (share * nj)
    wanted = ((block * q + which // n_s) * n_s + lax.rem(which, n_s)) * share + element
    perm[...] = jnp.where(place_col == wanted, 1.0, 0.0).astype(BF16)

    fields_two = field_moves(0)
    fields_one = field_moves(1)
    turn(h_ref, 0)
    for _, go, copy, _, _ in fields_two:
        when(go, lambda copy=copy: copy().start())
    turn(f_ref, 1)
    for _, go, copy, _, _ in fields_one:
        when(go, lambda copy=copy: copy().start())

    take_moves(moves_two, ("near",))
    fill_near(0)
    conv(0, k2_ref)

    totals = group_sums(sums_finish(0, r0), per) / members
    mean_one, mean_two = totals[0:1], totals[2:3]
    vec[0:1] = mean_one
    vec[1:2] = lax.rsqrt(totals[1:2] - mean_one * mean_one + EPS)
    vec[2:3] = gain_ref[0:1]
    vec[3:4] = mean_two
    vec[4:5] = lax.rsqrt(totals[3:4] - mean_two * mean_two + EPS)
    vec[5:6] = gain_ref[1:2]
    vec[6:8] = jnp.zeros((2, channels), F32)

    norm_back(h_ref, 3, 0)
    send_moves(moves_two, ("far",))
    take_fields(fields_two)
    across(0).start()
    gh[...] = norm_end(h_ref, 3, 0, 1).astype(BF16).reshape(frames, height, padded, half)
    send_moves(moves_one, ("near", "side"))
    send_moves(moves_one, ("far",))
    grads[1, own_frames, own_rows] = gh[...]

    across_land(0).wait_recv()
    activate(0, 3)
    take_moves(moves_two, ("side", "far"))
    fill_far(0)
    delta(0, d2_ref)
    take_fields(fields_one)
    across(1).start()

    take_moves(moves_one, ("near",))
    fill_near(1)
    conv(1, k1_ref)
    across_land(1).wait_recv()
    activate(1, 0)
    norm_back(f_ref, 0, 1)
    take_moves(moves_one, ("side", "far"))
    fill_far(1)
    delta(1, d1_ref)
    grad = norm_end(f_ref, 0, 1, 0)
    fg_ref[...] = (cot_ref[:, :, :, mine].reshape(rows, half).astype(F32) + grad).astype(BF16)

    for layer, own in ((0, d2_ref), (1, d1_ref)):
        for k in range(1, nj):
            for b in range(3):
                block_copy(layer, k, b).wait_recv()
                for a in range(3):
                    more = got[layer, k, b, a].astype(F32)
                    for c in range(3):
                        own[a * 9 + b * 3 + c] += more[:, c * half : (c + 1) * half]

    end_moves(moves_two)
    end_moves(moves_one)
    for found in (fields_two, fields_one):
        for _, go, copy, _, _ in found:
            when(go, lambda copy=copy: copy().wait_send())
    sums_end(0, r0)
    sums_end(1, r2)
    sums_end(2, r1)
    for layer in range(2):
        cross(layer).wait_send()
        across(layer).wait_send()
        for k in range(1, nj):
            for b in range(3):
                block_copy(layer, k, b).wait_send()


def shards(n_t, n_s, features, hidden, cotangent, kernel_one, kernel_two, gains):
    frames, height, width, channels = features.shape
    half = kernel_one.shape[4]
    padded = -(-width // 16) * 16
    if padded < width + 1:
        padded += 16
    q = 2 if n_t % 2 == 0 else 1
    n = n_t * n_s
    nj = n_t // q
    share = channels // n
    cs = channels // (q * n_s)
    rows = frames * height * padded
    lanes = height * padded
    tall = n_s * height

    def wide(field):
        return jnp.pad(field, ((0, 0), (0, 0), (0, padded - width), (0, 0)))

    def stacked(kernel):
        return kernel.transpose(1, 2, 3, 0, 4).reshape(9, 3, channels, half)

    vmem = pl.BlockSpec(memory_space=pltpu.VMEM)
    hbm = pl.BlockSpec(memory_space=pl.ANY)
    dma = pltpu.SemaphoreType.DMA
    around = 2 * n_s - 1
    grad, delta_one, delta_two, weighted = pl.pallas_call(
        functools.partial(body, (width, n_t, n_s, q)),
        out_shape=(
            jax.ShapeDtypeStruct((rows, half), BF16),
            jax.ShapeDtypeStruct((27, share, half), F32),
            jax.ShapeDtypeStruct((27, share, half), F32),
            jax.ShapeDtypeStruct((2, half), F32),
        ),
        in_specs=[vmem, vmem, vmem, hbm, hbm, vmem],
        out_specs=(vmem,) * 4,
        scratch_shapes=[
            pltpu.VMEM((2, q * frames + 2, tall, padded, half), BF16),
            pltpu.VMEM((2, q * frames + 2, tall + 2, padded, 3 * half), BF16),
            pltpu.VMEM((frames, height, padded, half), BF16),
            pltpu.VMEM((2, 9, channels, 3 * half), BF16),
            pltpu.VMEM((2, frames, channels, lanes), BF16),
            pltpu.VMEM((2, q * frames + 2, cs, tall * padded), BF16),
            pltpu.VMEM((2, q * frames + 2, cs, tall * padded), BF16),
            pltpu.VMEM((rows, channels), F32),
            pltpu.VMEM((2, rows, half), BF16),
            pltpu.VMEM((2, rows, half), BF16),
            pltpu.VMEM((8, channels), F32),
            pltpu.VMEM((n, 8, channels), F32),
            pltpu.VMEM((n, 8, half), F32),
            pltpu.VMEM((n, 8, half), F32),
            pltpu.VMEM((2, nj, 3, 3, share, 3 * half), BF16),
            pltpu.VMEM((2, nj, 3, 3, share, 3 * half), BF16),
            pltpu.VMEM((channels, channels), BF16),
            dma((2, 3)),
            dma((2, n_s)), dma((2, n_s)),
            dma((2,)), dma((2,)),
            dma((2, 2)), dma((2, 2)),
            dma((2, around)), dma((2, around)),
            dma((2, around)), dma((2, around)),
            dma((2, q, n_s)), dma((2, q, n_s)),
            dma((2, q, n_s)), dma((2, n_s)),
            dma((2,)), dma((2,)),
            dma((2, nj, 3)), dma((2, nj, 3)),
            dma((2,)), dma((2,)),
            dma((3, n)), dma((3, n)),
        ],
        compiler_params=pltpu.CompilerParams(
            collective_id=0, has_side_effects=True, vmem_limit_bytes=63 * 1024 * 1024
        ),
    )(wide(features), wide(hidden), wide(cotangent), stacked(kernel_one), stacked(kernel_two), gains)

    def unstacked(delta):
        return delta.reshape(3, 3, 3, share, half).transpose(3, 0, 1, 2, 4)

    feature_grad = grad.reshape(frames, height, padded, half)[:, :, :width]
    return (feature_grad, unstacked(delta_one), unstacked(delta_two), weighted)


def solution(mesh):
    placed = (
        P(("clip", "tm"), "space", None, None),
        P(("clip", "tm"), "space", None, None),
        P(("clip", "tm"), "space", None, None),
        P(None, None, None, None, "chan"),
        P(None, None, None, None, "chan"),
        P(),
    )
    return jax.shard_map(
        functools.partial(shards, mesh.shape["tm"], mesh.shape["space"]),
        mesh=mesh,
        in_specs=placed,
        out_specs=(
            P(("clip", "tm"), "space", None, "chan"),
            P(("clip", "tm", "space"), None, None, None, "chan"),
            P(("clip", "tm", "space"), None, None, None, "chan"),
            P("clip", "chan"),
        ),
        check_vma=False,
    )
```

```python
import functools

import jax
import jax.numpy as jnp
from jax import lax
from jax.experimental import pallas as pl
from jax.experimental.pallas import tpu as pltpu
from jax.sharding import PartitionSpec as P

GROUPS = 32
EPS = 1e-06
MESH = pl.DeviceIdType.MESH
F32 = jnp.float32
BF16 = jnp.bfloat16


def group_sums(values, per):
    channels = values.shape[1]
    row = lax.broadcasted_iota(jnp.int32, (channels, channels), 0) // per
    col = lax.broadcasted_iota(jnp.int32, (channels, channels), 1) // per
    same = jnp.where(row == col, 1.0, 0.0).astype(F32)
    return jnp.dot(values, same, precision=lax.Precision.HIGHEST, preferred_element_type=F32)


def body(
    sizes,
    f_ref, h_ref, cot_ref, k1_ref, k2_ref, gain_ref,
    fg_ref, d1_ref, d2_ref, w_ref,
    grads, hop, taps, gh, kcat, turned, raw, act, acc, xs, xr, vec, r0, r2, r1, out, got, perm,
    k_sem, gx_s, gx_r, gz_s, gz_r, ge_s, ge_r, gr_s, gr_r, gg_s, gg_r,
    ai_s, ai_r, an_s, an_r, ad_s, ad_r, dl_s, dl_r, xsem_s, xsem_r, ar_s, ar_r,
):
    width, n_t, n_s, q = sizes
    frames, height, padded, channels = cot_ref.shape
    half = channels // 2
    per = channels // GROUPS
    n = n_t * n_s
    nj = n_t // q
    rows = frames * height * padded
    lanes = height * padded
    tall = n_s * height
    share = channels // n
    cs = channels // (q * n_s)
    hc = cs // 2
    t = lax.axis_index("tm")
    s = lax.axis_index("space")
    chan = lax.axis_index("chan")
    partner = 1 - chan
    rank = t * n_s + s
    r = lax.rem(t, q)
    p = t // q
    members = float(frames * height * width * per * n)
    mine = pl.ds(pl.multiple_of(chan * half, half), half)
    theirs = pl.ds(pl.multiple_of(partner * half, half), half)
    own_rows = pl.ds(s * height, height)
    own_frames = pl.ds(r * frames, frames)
    next_frames = pl.ds((r + 1) * frames, frames)
    mate_frames = pl.ds((q - 1 - r) * frames, frames)
    sibling = {"chan": partner}

    def place(j):
        return {"tm": j // n_s, "space": lax.rem(j, n_s)}

    def peer(k):
        return lax.rem(rank + k, n)

    def each_peer(fn):
        def step(k, carry):
            fn(k)
            return carry

        lax.fori_loop(1, n, step, 0)

    def remote(src, dst, send, recv, device):
        return pltpu.make_async_remote_copy(
            src_ref=src, dst_ref=dst, send_sem=send, recv_sem=recv,
            device_id=device, device_id_type=MESH,
        )

    def kernel_copy(layer, source, c):
        return pltpu.make_async_copy(
            source.at[:, c], kcat.at[layer, :, :, c * half : (c + 1) * half], k_sem.at[layer, c]
        )

    for c in range(3):
        kernel_copy(0, k2_ref, c).start()
    for c in range(3):
        kernel_copy(1, k1_ref, c).start()

    barrier = pltpu.get_barrier_semaphore()
    pl.semaphore_signal(barrier, inc=1, device_id=sibling, device_id_type=MESH)
    each_peer(
        lambda k: pl.semaphore_signal(barrier, inc=1, device_id=place(peer(k)), device_id_type=MESH)
    )
    for layer in range(2):
        edge = jnp.zeros((q * frames + 2, 1, padded, 3 * half), BF16)
        taps[layer, :, 0:1] = edge
        taps[layer, :, tall + 1 : tall + 2] = edge

        @pl.when(t == n_t - 1)
        def _(layer=layer):
            def clear(f, carry):
                taps[layer, q * frames + f] = jnp.zeros((tall + 2, padded, 3 * half), BF16)
                return carry

            lax.fori_loop(0, 2, clear, 0)

    pl.semaphore_wait(barrier, n)

    def inside(value, count):
        return (value >= 0) & (value < count)

    def moves(layer, source):
        box = grads.at[layer]
        found = []
        before = jnp.where(r > 0, r, q) * frames
        sent = pl.ds(before, frames)

        def add(kind, go, src, dst, to, come, land, sender, send, recv):
            found.append((
                kind, go, lambda: remote(src, dst, send, recv, to),
                come, lambda: remote(land, land, send, recv, sender),
            ))

        for d, (ds, row) in enumerate(((1, height - 1), (-1, 0))):
            back = (s - ds) * height + row
            add(
                "near",
                (t > 0) & inside(s + ds, n_s),
                source.at[:, row : row + 1],
                box.at[sent, pl.ds(s * height + row, 1)],
                {"tm": t - 1, "space": s + ds},
                (t + 1 < n_t) & inside(s - ds, n_s),
                box.at[next_frames, pl.ds(back, 1)],
                {"tm": t + 1, "space": s - ds},
                ge_s.at[layer, d], ge_r.at[layer, d],
            )
        add(
            "near", t > 0, source, box.at[sent, own_rows], {"tm": t - 1},
            t + 1 < n_t, box.at[next_frames, own_rows], {"tm": t + 1},
            gz_s.at[layer], gz_r.at[layer],
        )
        for k in sorted((k for k in range(1 - n_s, n_s) if k), key=abs):
            i = k + n_s - 1
            spans = (("wide", 0, height),)
            if abs(k) == 1:
                spans = (("near x", height - 1, 1), ("wide", 0, height - 1))
                if k < 0:
                    spans = (("near x", 0, 1), ("wide", 1, height - 1))
            for part, (kind, low, count) in enumerate(spans):
                add(
                    kind, inside(s + k, n_s), source.at[:, low : low + count],
                    box.at[own_frames, pl.ds(s * height + low, count)], {"space": s + k},
                    inside(s - k, n_s),
                    box.at[own_frames, pl.ds((s - k) * height + low, count)], {"space": s - k},
                    gx_s.at[layer, part, i], gx_r.at[layer, part, i],
                )
        if q > 1:
            earlier = pl.ds((r - 1) * frames, frames)
            add(
                "side", r < q - 1, source, box.at[own_frames, own_rows], {"tm": t + 1},
                r > 0, box.at[earlier, own_rows], {"tm": t - 1},
                gg_s.at[layer], gg_r.at[layer],
            )
            for k in range(1, n_s):
                to, back = lax.rem(s + k, n_s), lax.rem(s + n_s - k, n_s)
                add(
                    "relay", None, box.at[mate_frames, own_rows], hop.at[layer, k], {"space": to},
                    None, hop.at[layer, k], {"space": back},
                    gr_s.at[layer, k], gr_r.at[layer, k],
                )
        return found

    def when(predicate, action):
        if predicate is None:
            action()
        else:
            pl.when(predicate)(action)

    def send_moves(found, kinds):
        for kind, go, copy, _, _ in found:
            if kind in kinds:
                when(go, lambda copy=copy: copy().start())

    def take_moves(found, kinds):
        for kind, _, _, come, copy in found:
            if kind in kinds:
                when(come, lambda copy=copy: copy().wait_recv())

    def end_moves(found):
        for _, go, copy, _, _ in found:
            when(go, lambda copy=copy: copy().wait_send())

    def set_rows(to_r, to_s):
        start = (to_r * n_s + to_s) * cs + chan * hc
        return pl.ds(pl.multiple_of(start, hc), hc)

    my_half = pl.ds(pl.multiple_of(chan * hc, hc), hc)

    def strip(at):
        return pl.ds(pl.multiple_of(at * lanes, lanes), lanes)

    def field_moves(layer):
        found = []
        for dr in range(q):
            for k in range(n_s):
                if dr == 0 and k == 0:
                    continue
                to_r, to_s = lax.rem(r + dr, q), lax.rem(s + k, n_s)
                from_r, from_s = lax.rem(r + q - dr, q), lax.rem(s + n_s - k, n_s)
                src = turned.at[layer, :, set_rows(to_r, to_s)]
                dst = raw.at[layer, pl.ds(2 + r * frames, frames), my_half, strip(s)]
                land = raw.at[layer, pl.ds(2 + from_r * frames, frames), my_half, strip(from_s)]
                sems = (ai_s.at[layer, dr, k], ai_r.at[layer, dr, k])
                found.append((
                    "in", None,
                    functools.partial(remote, src, dst, *sems, {"tm": p * q + to_r, "space": to_s}),
                    None,
                    functools.partial(remote, land, land, *sems, {"tm": p * q + from_r, "space": from_s}),
                ))
        for to_r in range(q):
            for k in range(n_s):
                to_s, from_s = lax.rem(s + k, n_s), lax.rem(s + n_s - k, n_s)
                src = turned.at[layer, frames - 2 : frames, set_rows(to_r, to_s)]
                dst = raw.at[layer, 0:2, my_half, strip(s)]
                land = raw.at[layer, 0:2, my_half, strip(from_s)]
                sems = (an_s.at[layer, to_r, k], an_r.at[layer, k])
                found.append((
                    "on", (r == q - 1) & (p + 1 < nj),
                    functools.partial(remote, src, dst, *sems, {"tm": (p + 1) * q + to_r, "space": to_s}),
                    (p > 0) if to_r == 0 else False,
                    functools.partial(remote, land, land, *sems, {"tm": p * q - 1, "space": from_s}),
                ))
        return found

    def take_fields(found):
        for _, _, _, come, copy in found:
            if come is not False:
                when(come, lambda copy=copy: copy().wait_recv())

    def across(layer):
        half_set = raw.at[layer, :, my_half]
        return remote(half_set, half_set, ad_s.at[layer], ad_r.at[layer], sibling)

    def across_land(layer):
        other = raw.at[layer, :, pl.ds(pl.multiple_of(partner * hc, hc), hc)]
        return remote(other, other, ad_s.at[layer], ad_r.at[layer], sibling)

    def sums_copy(layer, buf, k, slot):
        return remote(
            buf.at[slot], buf.at[slot], ar_s.at[layer, k], ar_r.at[layer, slot], place(peer(k))
        )

    def sums_start(layer, buf, values):
        buf[rank] = values
        each_peer(lambda k: sums_copy(layer, buf, k, rank).start())

    def sums_finish(layer, buf):
        each_peer(lambda k: sums_copy(layer, buf, k, peer(k)).wait_recv())
        return jnp.sum(buf[...], axis=0)

    def sums_end(layer, buf):
        each_peer(lambda k: sums_copy(layer, buf, k, rank).wait_send())

    def block_copy(layer, k, b):
        to = lax.rem(p + k, nj)
        return remote(
            out.at[layer, to, b], got.at[layer, k, b], dl_s.at[layer, k, b], dl_r.at[layer, k, b],
            {"tm": to * q + r},
        )

    def cross(layer):
        return remote(xs.at[layer], xr.at[layer], xsem_s.at[layer], xsem_r.at[layer], sibling)

    column = lax.rem(lax.broadcasted_iota(jnp.int32, (rows, 1), 0), padded)
    real = column < width

    def spread(layer, f, row, source):
        count = source.shape[0]
        cells = source.reshape(count * padded, half).astype(F32)
        size = count * padded
        ahead = pltpu.roll(cells, size - 1, 0)
        behind = pltpu.roll(cells, 1, 0)
        for c, value in enumerate((ahead, cells, behind)):
            taps[layer, f, pl.ds(row + 1, count), :, c * half : (c + 1) * half] = value.astype(
                BF16
            ).reshape(count, padded, half)

    def fill(layer, f, row, count):
        spread(layer, f, row, grads[layer, f, pl.ds(row, count)])

    def fill_rows(layer, first):
        for f in range(frames):
            fill(layer, first + f, s * height, height)
        for row, ok in ((s * height - 1, s > 0), ((s + 1) * height, s + 1 < n_s)):
            @pl.when(ok)
            def _(row=row):
                for f in range(frames):
                    fill(layer, first + f, row, 1)

    def fill_rest(layer):
        for k in range(1, n_s):
            back = lax.rem(s + n_s - k, n_s)
            for f in range(frames):
                fill(layer, r * frames + f, back * height, height)
                if q > 1:
                    mate = (q - 1 - r) * frames + f
                    spread(layer, mate, back * height, hop[layer, k, f])
        if q > 1:
            @pl.when(r > 0)
            def _():
                for f in range(frames):
                    fill(layer, f, s * height, height)

    def conv(layer, source, near):
        if near:
            for c in range(3):
                kernel_copy(layer, source, c).wait()
        for f in range(frames):
            total = None
            for ab in range(9):
                a, b = ab // 3, ab % 3
                if (2 - a + f < frames) != near:
                    continue
                left = taps[
                    layer, r * frames + (2 - a + f), pl.ds(s * height + (2 - b), height)
                ].reshape(lanes, 3 * half)
                term = lax.dot_general(
                    left, kcat[layer, ab], (((1,), (1,)), ((), ())), preferred_element_type=F32
                )
                total = term if total is None else total + term
            if total is None:
                continue
            if near:
                acc[f * lanes : (f + 1) * lanes] = total
            else:
                acc[f * lanes : (f + 1) * lanes] += total
        if not near:
            xs[layer] = acc[:, theirs].astype(BF16)
            cross(layer).start()

    def norm_back(field_ref, base, layer):
        cross(layer).wait_recv()
        upstream = acc[:, mine] + xr[layer].astype(F32)
        field = field_ref[:, :, :, mine].reshape(rows, half).astype(F32)
        scale = vec[base + 1 : base + 2, mine]
        gain = vec[base + 2 : base + 3, mine]
        centred = (field - vec[base : base + 1, mine]) * scale
        scaled = centred * gain
        gate = jax.nn.sigmoid(scaled)
        slope = jnp.where(real, upstream * gate * (1.0 + scaled * (1.0 - gate)), 0.0)
        acc[:, mine] = slope
        parts = [
            jnp.sum(slope, axis=0, keepdims=True),
            jnp.sum(slope * centred, axis=0, keepdims=True),
            jnp.zeros((6, half), F32),
        ]
        sums_start(layer + 1, (r2, r1)[layer], jnp.concatenate(parts, axis=0))

    def norm_end(field_ref, base, layer, w_row):
        totals = sums_finish(layer + 1, (r2, r1)[layer])
        w_ref[w_row : w_row + 1] = totals[1:2]
        scale = vec[base + 1 : base + 2, mine]
        gain = vec[base + 2 : base + 3, mine]
        means = group_sums(totals * gain, per) / members
        field = field_ref[:, :, :, mine].reshape(rows, half).astype(F32)
        centred = (field - vec[base : base + 1, mine]) * scale
        grad = scale * (acc[:, mine] * gain - means[0:1] - centred * means[1:2])
        return jnp.where(real, grad, 0.0)

    def turn(field_ref, layer):
        for f in range(frames):
            cells = field_ref[f].reshape(lanes, channels)
            flat = lax.dot_general(
                perm[...], cells, (((1,), (1,)), ((), ())), preferred_element_type=F32
            ).astype(BF16)
            turned[layer, f] = flat
        raw[layer, pl.ds(2 + r * frames, frames), my_half, strip(s)] = turned[layer, :, set_rows(r, s)]

    def activate(layer, base):
        pick = perm[pl.ds(pl.multiple_of((r * n_s + s) * cs, cs), cs)].astype(F32)
        cols = lax.dot_general(
            pick, vec[...], (((1,), (1,)), ((), ())),
            precision=lax.Precision.HIGHEST, preferred_element_type=F32,
        )
        mean, scale, gain = (cols[:, base + i : base + i + 1] for i in range(3))
        spot = lax.rem(lax.broadcasted_iota(jnp.int32, (1, tall * padded), 1), padded)

        def step(f, carry):
            field = raw[layer, f].astype(F32)
            scaled = (field - mean) * scale * gain
            keep = (spot < width) & ((f >= 2) | (p > 0))
            active = jnp.where(keep, scaled * jax.nn.sigmoid(scaled), 0.0)
            act[layer, f] = active.astype(BF16)
            return carry

        lax.fori_loop(0, q * frames + 2, step, 0)

    def delta(layer, own):
        for b in range(3):
            product = None
            for f in range(q * frames):
                left = act[layer, f : f + 3].reshape(3 * cs, tall * padded)
                right = taps[layer, f, 2 - b : 2 - b + tall].reshape(tall * padded, 3 * half)
                term = jnp.dot(left, right, preferred_element_type=F32)
                product = term if product is None else product + term
            small = product.astype(BF16)
            for j in range(nj):
                for a in range(3):
                    low = a * cs + j * share
                    out[layer, j, b, a] = small[low : low + share]

                @pl.when(p == j)
                def _(j=j):
                    for a in range(3):
                        low = a * cs + j * share
                        for c in range(3):
                            own[a * 9 + b * 3 + c] = product[
                                low : low + share, c * half : (c + 1) * half
                            ]

            for k in range(1, nj):
                block_copy(layer, k, b).start()

    moves_two = moves(0, cot_ref.at[:, :, :, mine])
    moves_one = moves(1, gh)
    send_moves(moves_two, ("near x", "near"))
    send_moves(moves_two, ("side", "wide"))
    grads[0, own_frames, own_rows] = cot_ref[:, :, :, mine]

    field_one = f_ref[...].reshape(rows, channels).astype(F32)
    field_two = h_ref[...].reshape(rows, channels).astype(F32)
    parts = [
        jnp.sum(field_one, axis=0, keepdims=True),
        jnp.sum(field_one * field_one, axis=0, keepdims=True),
        jnp.sum(field_two, axis=0, keepdims=True),
        jnp.sum(field_two * field_two, axis=0, keepdims=True),
        jnp.zeros((4, channels), F32),
    ]
    sums_start(0, r0, jnp.concatenate(parts, axis=0))

    place_row = lax.broadcasted_iota(jnp.int32, (channels, channels), 0)
    place_col = lax.broadcasted_iota(jnp.int32, (channels, channels), 1)
    element = lax.rem(place_row, share)
    block = lax.rem(place_row // share, nj)
    which = place_row // (share * nj)
    wanted = ((block * q + which // n_s) * n_s + lax.rem(which, n_s)) * share + element
    perm[...] = jnp.where(place_col == wanted, 1.0, 0.0).astype(BF16)

    fields_two = field_moves(0)
    fields_one = field_moves(1)

    def send_fields(found):
        for _, go, copy, _, _ in found:
            when(go, lambda copy=copy: copy().start())

    turn(h_ref, 0)
    send_fields(fields_two)
    turn(f_ref, 1)

    take_moves(moves_two, ("near x",))
    fill_rows(0, r * frames)
    conv(0, k2_ref, True)
    take_moves(moves_two, ("near", "side"))
    send_moves(moves_two, ("relay",))
    pl.when(t + 1 < n_t)(lambda: fill_rows(0, (r + 1) * frames))
    conv(0, k2_ref, False)

    totals = group_sums(sums_finish(0, r0), per) / members
    mean_one, mean_two = totals[0:1], totals[2:3]
    vec[0:1] = mean_one
    vec[1:2] = lax.rsqrt(totals[1:2] - mean_one * mean_one + EPS)
    vec[2:3] = gain_ref[0:1]
    vec[3:4] = mean_two
    vec[4:5] = lax.rsqrt(totals[3:4] - mean_two * mean_two + EPS)
    vec[5:6] = gain_ref[1:2]
    vec[6:8] = jnp.zeros((2, channels), F32)

    norm_back(h_ref, 3, 0)
    send_fields(fields_one)
    take_fields(fields_two)
    across(0).start()
    take_moves(moves_two, ("wide", "relay"))
    fill_rest(0)
    across_land(0).wait_recv()
    activate(0, 3)
    gh[...] = norm_end(h_ref, 3, 0, 1).astype(BF16).reshape(frames, height, padded, half)
    send_moves(moves_one, ("near x", "near"))
    send_moves(moves_one, ("side", "wide"))
    grads[1, own_frames, own_rows] = gh[...]

    delta(0, d2_ref)
    take_fields(fields_one)
    across(1).start()
    across_land(1).wait_recv()
    activate(1, 0)

    take_moves(moves_one, ("near x",))
    fill_rows(1, r * frames)
    conv(1, k1_ref, True)
    take_moves(moves_one, ("near", "side"))
    send_moves(moves_one, ("relay",))
    pl.when(t + 1 < n_t)(lambda: fill_rows(1, (r + 1) * frames))
    conv(1, k1_ref, False)
    norm_back(f_ref, 0, 1)
    take_moves(moves_one, ("wide", "relay"))
    fill_rest(1)
    delta(1, d1_ref)
    grad = norm_end(f_ref, 0, 1, 0)
    fg_ref[...] = (cot_ref[:, :, :, mine].reshape(rows, half).astype(F32) + grad).astype(BF16)

    for layer, own in ((0, d2_ref), (1, d1_ref)):
        for k in range(1, nj):
            for b in range(3):
                block_copy(layer, k, b).wait_recv()
                for a in range(3):
                    more = got[layer, k, b, a].astype(F32)
                    for c in range(3):
                        own[a * 9 + b * 3 + c] += more[:, c * half : (c + 1) * half]

    end_moves(moves_two)
    end_moves(moves_one)
    for found in (fields_two, fields_one):
        for _, go, copy, _, _ in found:
            when(go, lambda copy=copy: copy().wait_send())
    sums_end(0, r0)
    sums_end(1, r2)
    sums_end(2, r1)
    for layer in range(2):
        cross(layer).wait_send()
        across(layer).wait_send()
        for k in range(1, nj):
            for b in range(3):
                block_copy(layer, k, b).wait_send()


def shards(n_t, n_s, features, hidden, cotangent, kernel_one, kernel_two, gains):
    frames, height, width, channels = features.shape
    half = kernel_one.shape[4]
    padded = -(-width // 16) * 16
    if padded < width + 1:
        padded += 16
    q = 2 if n_t % 2 == 0 else 1
    n = n_t * n_s
    nj = n_t // q
    share = channels // n
    cs = channels // (q * n_s)
    rows = frames * height * padded
    lanes = height * padded
    tall = n_s * height

    def wide(field):
        return jnp.pad(field, ((0, 0), (0, 0), (0, padded - width), (0, 0)))

    def stacked(kernel):
        return kernel.transpose(1, 2, 3, 0, 4).reshape(9, 3, channels, half)

    vmem = pl.BlockSpec(memory_space=pltpu.VMEM)
    hbm = pl.BlockSpec(memory_space=pl.ANY)
    dma = pltpu.SemaphoreType.DMA
    around = 2 * n_s - 1
    grad, delta_one, delta_two, weighted = pl.pallas_call(
        functools.partial(body, (width, n_t, n_s, q)),
        out_shape=(
            jax.ShapeDtypeStruct((rows, half), BF16),
            jax.ShapeDtypeStruct((27, share, half), F32),
            jax.ShapeDtypeStruct((27, share, half), F32),
            jax.ShapeDtypeStruct((2, half), F32),
        ),
        in_specs=[vmem, vmem, vmem, hbm, hbm, vmem],
        out_specs=(vmem,) * 4,
        scratch_shapes=[
            pltpu.VMEM((2, q * frames + 2, tall, padded, half), BF16),
            pltpu.VMEM((2, n_s, frames, height, padded, half), BF16),
            pltpu.VMEM((2, q * frames + 2, tall + 2, padded, 3 * half), BF16),
            pltpu.VMEM((frames, height, padded, half), BF16),
            pltpu.VMEM((2, 9, channels, 3 * half), BF16),
            pltpu.VMEM((2, frames, channels, lanes), BF16),
            pltpu.VMEM((2, q * frames + 2, cs, tall * padded), BF16),
            pltpu.VMEM((2, q * frames + 2, cs, tall * padded), BF16),
            pltpu.VMEM((rows, channels), F32),
            pltpu.VMEM((2, rows, half), BF16),
            pltpu.VMEM((2, rows, half), BF16),
            pltpu.VMEM((8, channels), F32),
            pltpu.VMEM((n, 8, channels), F32),
            pltpu.VMEM((n, 8, half), F32),
            pltpu.VMEM((n, 8, half), F32),
            pltpu.VMEM((2, nj, 3, 3, share, 3 * half), BF16),
            pltpu.VMEM((2, nj, 3, 3, share, 3 * half), BF16),
            pltpu.VMEM((channels, channels), BF16),
            dma((2, 3)),
            dma((2, 2, around)), dma((2, 2, around)),
            dma((2,)), dma((2,)),
            dma((2, 2)), dma((2, 2)),
            dma((2, n_s)), dma((2, n_s)),
            dma((2,)), dma((2,)),
            dma((2, q, n_s)), dma((2, q, n_s)),
            dma((2, q, n_s)), dma((2, n_s)),
            dma((2,)), dma((2,)),
            dma((2, nj, 3)), dma((2, nj, 3)),
            dma((2,)), dma((2,)),
            dma((3, n)), dma((3, n)),
        ],
        compiler_params=pltpu.CompilerParams(
            collective_id=0, has_side_effects=True, vmem_limit_bytes=40 * 1024 * 1024
        ),
    )(wide(features), wide(hidden), wide(cotangent), stacked(kernel_one), stacked(kernel_two), gains)

    def unstacked(delta):
        return delta.reshape(3, 3, 3, share, half).transpose(3, 0, 1, 2, 4)

    feature_grad = grad.reshape(frames, height, padded, half)[:, :, :width]
    return (feature_grad, unstacked(delta_one), unstacked(delta_two), weighted)


def solution(mesh):
    placed = (
        P(("clip", "tm"), "space", None, None),
        P(("clip", "tm"), "space", None, None),
        P(("clip", "tm"), "space", None, None),
        P(None, None, None, None, "chan"),
        P(None, None, None, None, "chan"),
        P(),
    )
    return jax.shard_map(
        functools.partial(shards, mesh.shape["tm"], mesh.shape["space"]),
        mesh=mesh,
        in_specs=placed,
        out_specs=(
            P(("clip", "tm"), "space", None, "chan"),
            P(("clip", "tm", "space"), None, None, None, "chan"),
            P(("clip", "tm", "space"), None, None, None, "chan"),
            P("clip", "chan"),
        ),
        check_vma=False,
    )
```

```python
import functools

import jax
import jax.numpy as jnp
from jax import lax
from jax.experimental import pallas as pl
from jax.experimental.pallas import tpu as pltpu
from jax.sharding import PartitionSpec as P

GROUPS = 32
EPS = 1e-06
MESH = pl.DeviceIdType.MESH
F32 = jnp.float32
BF16 = jnp.bfloat16


def group_sums(values, per):
    channels = values.shape[1]
    row = lax.broadcasted_iota(jnp.int32, (channels, channels), 0) // per
    col = lax.broadcasted_iota(jnp.int32, (channels, channels), 1) // per
    same = jnp.where(row == col, 1.0, 0.0).astype(F32)
    return jnp.dot(values, same, precision=lax.Precision.HIGHEST, preferred_element_type=F32)


def body(
    sizes,
    f_ref, h_ref, cot_ref, k1_ref, k2_ref, gain_ref,
    fg_ref, d1_ref, d2_ref, w_ref,
    fg, mixed, d1, d2, weights, o_sem,
    grads, hop, taps, gh, kcat, turned, raw, act, acc, xs, xr, vec, r0, r2, r1, out, got, perm,
    k_sem, gx_s, gx_r, gz_s, gz_r, ge_s, ge_r, gr_s, gr_r, gg_s, gg_r,
    ai_s, ai_r, an_s, an_r, ad_s, ad_r, dl_s, dl_r, xsem_s, xsem_r, ar_s, ar_r,
):
    width, n_t, n_s, q = sizes
    frames, height, padded, channels = cot_ref.shape
    half = channels // 2
    per = channels // GROUPS
    n = n_t * n_s
    nj = n_t // q
    rows = frames * height * padded
    lanes = height * padded
    tall = n_s * height
    share = channels // n
    cs = channels // (q * n_s)
    hc = cs // 2
    t = lax.axis_index("tm")
    s = lax.axis_index("space")
    chan = lax.axis_index("chan")
    partner = 1 - chan
    rank = t * n_s + s
    r = lax.rem(t, q)
    p = t // q
    members = float(frames * height * width * per * n)
    mine = pl.ds(pl.multiple_of(chan * half, half), half)
    theirs = pl.ds(pl.multiple_of(partner * half, half), half)
    own_rows = pl.ds(s * height, height)
    own_frames = pl.ds(r * frames, frames)
    next_frames = pl.ds((r + 1) * frames, frames)
    sibling = {"chan": partner}

    def place(j):
        return {"tm": j // n_s, "space": lax.rem(j, n_s)}

    def peer(k):
        return lax.rem(rank + k, n)

    def each_peer(fn):
        def step(k, carry):
            fn(k)
            return carry

        lax.fori_loop(1, n, step, 0)

    def remote(src, dst, send, recv, device):
        return pltpu.make_async_remote_copy(
            src_ref=src, dst_ref=dst, send_sem=send, recv_sem=recv,
            device_id=device, device_id_type=MESH,
        )

    def kernel_copy(layer, source, c):
        return pltpu.make_async_copy(
            source.at[:, c], kcat.at[layer, :, :, c * half : (c + 1) * half], k_sem.at[layer, c]
        )

    for c in range(3):
        kernel_copy(0, k2_ref, c).start()
    for c in range(3):
        kernel_copy(1, k1_ref, c).start()

    barrier = pltpu.get_barrier_semaphore()
    pl.semaphore_signal(barrier, inc=1, device_id=sibling, device_id_type=MESH)
    each_peer(
        lambda k: pl.semaphore_signal(barrier, inc=1, device_id=place(peer(k)), device_id_type=MESH)
    )
    for layer in range(2):
        edge = jnp.zeros((q * frames + 2, 1, padded, 3 * half), BF16)
        taps[layer, :, 0:1] = edge
        taps[layer, :, tall + 1 : tall + 2] = edge

        @pl.when(t == n_t - 1)
        def _(layer=layer):
            def clear(f, carry):
                taps[layer, q * frames + f] = jnp.zeros((tall + 2, padded, 3 * half), BF16)
                return carry

            lax.fori_loop(0, 2, clear, 0)

    pl.semaphore_wait(barrier, n)

    def inside(value, count):
        return (value >= 0) & (value < count)

    def moves(layer, source):
        box = grads.at[layer]
        found = []
        before = jnp.where(r > 0, r, q) * frames
        sent = pl.ds(before, frames)

        def add(kind, go, src, dst, to, come, land, sender, send, recv):
            found.append((
                kind, go, lambda: remote(src, dst, send, recv, to),
                come, lambda: remote(land, land, send, recv, sender),
            ))

        for d, (ds, row) in enumerate(((1, height - 1), (-1, 0))):
            back = (s - ds) * height + row
            add(
                "near",
                (t > 0) & inside(s + ds, n_s),
                source.at[:, row : row + 1],
                box.at[sent, pl.ds(s * height + row, 1)],
                {"tm": t - 1, "space": s + ds},
                (t + 1 < n_t) & inside(s - ds, n_s),
                box.at[next_frames, pl.ds(back, 1)],
                {"tm": t + 1, "space": s - ds},
                ge_s.at[layer, d], ge_r.at[layer, d],
            )
        add(
            "near", t > 0, source, box.at[sent, own_rows], {"tm": t - 1},
            t + 1 < n_t, box.at[next_frames, own_rows], {"tm": t + 1},
            gz_s.at[layer], gz_r.at[layer],
        )
        for k in sorted((k for k in range(1 - n_s, n_s) if k), key=abs):
            i = k + n_s - 1
            spans = (("wide", 0, height),)
            if abs(k) == 1:
                spans = (("near x", height - 1, 1), ("wide", 0, height - 1))
                if k < 0:
                    spans = (("near x", 0, 1), ("wide", 1, height - 1))
            for part, (kind, low, count) in enumerate(spans):
                add(
                    kind, inside(s + k, n_s), source.at[:, low : low + count],
                    box.at[own_frames, pl.ds(s * height + low, count)], {"space": s + k},
                    inside(s - k, n_s),
                    box.at[own_frames, pl.ds((s - k) * height + low, count)], {"space": s - k},
                    gx_s.at[layer, part, i], gx_r.at[layer, part, i],
                )
        if q > 1:
            earlier = pl.ds((r - 1) * frames, frames)
            add(
                "side", r < q - 1, source, box.at[own_frames, own_rows], {"tm": t + 1},
                r > 0, box.at[earlier, own_rows], {"tm": t - 1},
                gg_s.at[layer], gg_r.at[layer],
            )
            for k in range(1, n_s):
                to, back = lax.rem(s + k, n_s), lax.rem(s + n_s - k, n_s)
                for f in range(frames):
                    add(
                        "relay" if f == 0 else "relay on",
                        None, box.at[(q - 1 - r) * frames + f, own_rows], hop.at[layer, k, f],
                        {"space": to},
                        None, hop.at[layer, k, f], {"space": back},
                        gr_s.at[layer, f, k], gr_r.at[layer, f, k],
                    )
        return found

    def when(predicate, action):
        if predicate is None:
            action()
        else:
            pl.when(predicate)(action)

    def send_moves(found, kinds):
        for kind, go, copy, _, _ in found:
            if kind in kinds:
                when(go, lambda copy=copy: copy().start())

    def take_moves(found, kinds):
        for kind, _, _, come, copy in found:
            if kind in kinds:
                when(come, lambda copy=copy: copy().wait_recv())

    def end_moves(found):
        for _, go, copy, _, _ in found:
            when(go, lambda copy=copy: copy().wait_send())

    def set_rows(to_r, to_s):
        start = (to_r * n_s + to_s) * cs + chan * hc
        return pl.ds(pl.multiple_of(start, hc), hc)

    my_half = pl.ds(pl.multiple_of(chan * hc, hc), hc)

    def strip(at):
        return pl.ds(pl.multiple_of(at * lanes, lanes), lanes)

    def field_moves(layer):
        found = []
        for dr in range(q):
            for k in range(n_s):
                if dr == 0 and k == 0:
                    continue
                to_r, to_s = lax.rem(r + dr, q), lax.rem(s + k, n_s)
                from_r, from_s = lax.rem(r + q - dr, q), lax.rem(s + n_s - k, n_s)
                src = turned.at[layer, :, set_rows(to_r, to_s)]
                dst = raw.at[layer, pl.ds(2 + r * frames, frames), my_half, strip(s)]
                land = raw.at[layer, pl.ds(2 + from_r * frames, frames), my_half, strip(from_s)]
                sems = (ai_s.at[layer, dr, k], ai_r.at[layer, dr, k])
                found.append((
                    "in", None,
                    functools.partial(remote, src, dst, *sems, {"tm": p * q + to_r, "space": to_s}),
                    None,
                    functools.partial(remote, land, land, *sems, {"tm": p * q + from_r, "space": from_s}),
                ))
        for to_r in range(q):
            for k in range(n_s):
                to_s, from_s = lax.rem(s + k, n_s), lax.rem(s + n_s - k, n_s)
                src = turned.at[layer, frames - 2 : frames, set_rows(to_r, to_s)]
                dst = raw.at[layer, 0:2, my_half, strip(s)]
                land = raw.at[layer, 0:2, my_half, strip(from_s)]
                sems = (an_s.at[layer, to_r, k], an_r.at[layer, k])
                found.append((
                    "on", (r == q - 1) & (p + 1 < nj),
                    functools.partial(remote, src, dst, *sems, {"tm": (p + 1) * q + to_r, "space": to_s}),
                    (p > 0) if to_r == 0 else False,
                    functools.partial(remote, land, land, *sems, {"tm": p * q - 1, "space": from_s}),
                ))
        return found

    def take_fields(found):
        for _, _, _, come, copy in found:
            if come is not False:
                when(come, lambda copy=copy: copy().wait_recv())

    def across(layer):
        half_set = raw.at[layer, :, my_half]
        return remote(half_set, half_set, ad_s.at[layer], ad_r.at[layer], sibling)

    def across_land(layer):
        other = raw.at[layer, :, pl.ds(pl.multiple_of(partner * hc, hc), hc)]
        return remote(other, other, ad_s.at[layer], ad_r.at[layer], sibling)

    def sums_copy(layer, buf, k, slot):
        return remote(
            buf.at[slot], buf.at[slot], ar_s.at[layer, k], ar_r.at[layer, slot], place(peer(k))
        )

    def sums_start(layer, buf, values):
        buf[rank] = values
        each_peer(lambda k: sums_copy(layer, buf, k, rank).start())

    def sums_finish(layer, buf):
        each_peer(lambda k: sums_copy(layer, buf, k, peer(k)).wait_recv())
        return jnp.sum(buf[...], axis=0)

    def sums_end(layer, buf):
        each_peer(lambda k: sums_copy(layer, buf, k, rank).wait_send())

    def block_copy(layer, k, b):
        to = lax.rem(p + k, nj)
        return remote(
            out.at[layer, to, b], got.at[layer, k, b], dl_s.at[layer, k, b], dl_r.at[layer, k, b],
            {"tm": to * q + r},
        )

    def cross(layer):
        return remote(xs.at[layer], xr.at[layer], xsem_s.at[layer], xsem_r.at[layer], sibling)

    column = lax.rem(lax.broadcasted_iota(jnp.int32, (rows, 1), 0), padded)
    real = column < width

    def spread(layer, f, row, source):
        count = source.shape[0]
        cells = source.reshape(count * padded, half).astype(F32)
        size = count * padded
        ahead = pltpu.roll(cells, size - 1, 0)
        behind = pltpu.roll(cells, 1, 0)
        for c, value in enumerate((ahead, cells, behind)):
            taps[layer, f, pl.ds(row + 1, count), :, c * half : (c + 1) * half] = value.astype(
                BF16
            ).reshape(count, padded, half)

    def fill(layer, f, row, count):
        spread(layer, f, row, grads[layer, f, pl.ds(row, count)])

    def fill_rows(layer, first):
        for f in range(frames):
            fill(layer, first + f, s * height, height)
        for row, ok in ((s * height - 1, s > 0), ((s + 1) * height, s + 1 < n_s)):
            @pl.when(ok)
            def _(row=row):
                for f in range(frames):
                    fill(layer, first + f, row, 1)

    def fill_rest(layer):
        for k in range(1, n_s):
            back = lax.rem(s + n_s - k, n_s)
            for f in range(frames):
                fill(layer, r * frames + f, back * height, height)
                if q > 1:
                    mate = (q - 1 - r) * frames + f
                    spread(layer, mate, back * height, hop[layer, k, f])
        if q > 1:
            @pl.when(r > 0)
            def _():
                for f in range(frames):
                    fill(layer, f, s * height, height)

    def conv(layer, source, near):
        if near:
            for c in range(3):
                kernel_copy(layer, source, c).wait()
        for f in range(frames):
            total = None
            for ab in range(9):
                a, b = ab // 3, ab % 3
                if (2 - a + f < frames) != near:
                    continue
                left = taps[
                    layer, r * frames + (2 - a + f), pl.ds(s * height + (2 - b), height)
                ].reshape(lanes, 3 * half)
                term = lax.dot_general(
                    left, kcat[layer, ab], (((1,), (1,)), ((), ())), preferred_element_type=F32
                )
                total = term if total is None else total + term
            if total is None:
                continue
            if near:
                acc[f * lanes : (f + 1) * lanes] = total
            else:
                acc[f * lanes : (f + 1) * lanes] += total
        if not near:
            xs[layer] = acc[:, theirs].astype(BF16)
            cross(layer).start()

    def norm_back(field_ref, base, layer):
        cross(layer).wait_recv()
        upstream = acc[:, mine] + xr[layer].astype(F32)
        field = field_ref[:, :, :, mine].reshape(rows, half).astype(F32)
        scale = vec[base + 1 : base + 2, mine]
        gain = vec[base + 2 : base + 3, mine]
        centred = (field - vec[base : base + 1, mine]) * scale
        scaled = centred * gain
        gate = jax.nn.sigmoid(scaled)
        slope = jnp.where(real, upstream * gate * (1.0 + scaled * (1.0 - gate)), 0.0)
        acc[:, mine] = slope
        parts = [
            jnp.sum(slope, axis=0, keepdims=True),
            jnp.sum(slope * centred, axis=0, keepdims=True),
            jnp.zeros((6, half), F32),
        ]
        sums_start(layer + 1, (r2, r1)[layer], jnp.concatenate(parts, axis=0))

    def norm_end(field_ref, base, layer, w_row):
        totals = sums_finish(layer + 1, (r2, r1)[layer])
        weights[w_row : w_row + 1] = totals[1:2]
        scale = vec[base + 1 : base + 2, mine]
        gain = vec[base + 2 : base + 3, mine]
        means = group_sums(totals * gain, per) / members
        field = field_ref[:, :, :, mine].reshape(rows, half).astype(F32)
        centred = (field - vec[base : base + 1, mine]) * scale
        grad = scale * (acc[:, mine] * gain - means[0:1] - centred * means[1:2])
        return jnp.where(real, grad, 0.0)

    def turn(field_ref, layer):
        for f in range(frames):
            cells = field_ref[f].reshape(lanes, channels)
            flat = lax.dot_general(
                perm[...], cells, (((1,), (1,)), ((), ())), preferred_element_type=F32
            ).astype(BF16)
            turned[layer, f] = flat
        raw[layer, pl.ds(2 + r * frames, frames), my_half, strip(s)] = turned[layer, :, set_rows(r, s)]

    def activate(layer, base):
        pick = perm[pl.ds(pl.multiple_of((r * n_s + s) * cs, cs), cs)].astype(F32)
        cols = lax.dot_general(
            pick, vec[...], (((1,), (1,)), ((), ())),
            precision=lax.Precision.HIGHEST, preferred_element_type=F32,
        )
        mean, scale, gain = (cols[:, base + i : base + i + 1] for i in range(3))
        spot = lax.rem(lax.broadcasted_iota(jnp.int32, (1, tall * padded), 1), padded)

        def step(f, carry):
            field = raw[layer, f].astype(F32)
            scaled = (field - mean) * scale * gain
            keep = (spot < width) & ((f >= 2) | (p > 0))
            active = jnp.where(keep, scaled * jax.nn.sigmoid(scaled), 0.0)
            act[layer, f] = active.astype(BF16)
            return carry

        lax.fori_loop(0, q * frames + 2, step, 0)

    def delta(layer, own):
        for b in range(3):
            product = None
            for f in range(q * frames):
                left = act[layer, f : f + 3].reshape(3 * cs, tall * padded)
                right = taps[layer, f, 2 - b : 2 - b + tall].reshape(tall * padded, 3 * half)
                term = jnp.dot(left, right, preferred_element_type=F32)
                product = term if product is None else product + term
            small = product.astype(BF16)
            for j in range(nj):
                for a in range(3):
                    low = a * cs + j * share
                    out[layer, j, b, a] = small[low : low + share]

                @pl.when(p == j)
                def _(j=j):
                    for a in range(3):
                        low = a * cs + j * share
                        for c in range(3):
                            own[a, b, c] = product[
                                low : low + share, c * half : (c + 1) * half
                            ]

            for k in range(1, nj):
                block_copy(layer, k, b).start()

    moves_two = moves(0, cot_ref.at[:, :, :, mine])
    moves_one = moves(1, gh)
    send_moves(moves_two, ("near x", "near"))
    send_moves(moves_two, ("side", "wide"))
    grads[0, own_frames, own_rows] = cot_ref[:, :, :, mine]

    field_one = f_ref[...].reshape(rows, channels).astype(F32)
    field_two = h_ref[...].reshape(rows, channels).astype(F32)
    parts = [
        jnp.sum(field_one, axis=0, keepdims=True),
        jnp.sum(field_one * field_one, axis=0, keepdims=True),
        jnp.sum(field_two, axis=0, keepdims=True),
        jnp.sum(field_two * field_two, axis=0, keepdims=True),
        jnp.zeros((4, channels), F32),
    ]
    sums_start(0, r0, jnp.concatenate(parts, axis=0))

    place_row = lax.broadcasted_iota(jnp.int32, (channels, channels), 0)
    place_col = lax.broadcasted_iota(jnp.int32, (channels, channels), 1)
    element = lax.rem(place_row, share)
    block = lax.rem(place_row // share, nj)
    which = place_row // (share * nj)
    wanted = ((block * q + which // n_s) * n_s + lax.rem(which, n_s)) * share + element
    perm[...] = jnp.where(place_col == wanted, 1.0, 0.0).astype(BF16)

    fields_two = field_moves(0)
    fields_one = field_moves(1)

    def send_fields(found):
        for _, go, copy, _, _ in found:
            when(go, lambda copy=copy: copy().start())

    turn(h_ref, 0)
    turn(f_ref, 1)

    take_moves(moves_two, ("near x",))
    fill_rows(0, r * frames)
    conv(0, k2_ref, True)
    take_moves(moves_two, ("near", "side"))
    send_fields(fields_two)
    send_moves(moves_two, ("relay",))
    pl.when(t + 1 < n_t)(lambda: fill_rows(0, (r + 1) * frames))
    conv(0, k2_ref, False)

    totals = group_sums(sums_finish(0, r0), per) / members
    mean_one, mean_two = totals[0:1], totals[2:3]
    vec[0:1] = mean_one
    vec[1:2] = lax.rsqrt(totals[1:2] - mean_one * mean_one + EPS)
    vec[2:3] = gain_ref[0:1]
    vec[3:4] = mean_two
    vec[4:5] = lax.rsqrt(totals[3:4] - mean_two * mean_two + EPS)
    vec[5:6] = gain_ref[1:2]
    vec[6:8] = jnp.zeros((2, channels), F32)

    norm_back(h_ref, 3, 0)
    send_moves(moves_two, ("relay on",))
    send_fields(fields_one)
    gh[...] = norm_end(h_ref, 3, 0, 1).astype(BF16).reshape(frames, height, padded, half)
    send_moves(moves_one, ("near x", "near"))
    send_moves(moves_one, ("side", "wide"))
    grads[1, own_frames, own_rows] = gh[...]

    take_fields(fields_two)
    across(0).start()
    take_moves(moves_two, ("wide", "relay", "relay on"))
    fill_rest(0)
    across_land(0).wait_recv()
    activate(0, 3)
    delta(0, d2)
    take_moves(moves_one, ("near x",))
    fill_rows(1, r * frames)
    conv(1, k1_ref, True)
    take_moves(moves_one, ("near", "side"))
    send_moves(moves_one, ("relay", "relay on"))
    pl.when(t + 1 < n_t)(lambda: fill_rows(1, (r + 1) * frames))
    conv(1, k1_ref, False)
    take_fields(fields_one)
    across(1).start()
    norm_back(f_ref, 0, 1)
    across_land(1).wait_recv()
    activate(1, 0)
    take_moves(moves_one, ("wide", "relay", "relay on"))
    fill_rest(1)
    delta(1, d1)
    grad = norm_end(f_ref, 0, 1, 0)
    total = cot_ref[:, :, :, mine].reshape(rows, half).astype(F32) + grad
    for f in range(frames):
        for h in range(height):
            at = (f * height + h) * padded
            mixed[f, pl.ds(h, width, stride=height)] = total[at : at + width]
    fg[...] = mixed[...].astype(BF16)
    results = [
        pltpu.make_async_copy(fg, fg_ref, o_sem.at[0]),
        pltpu.make_async_copy(weights, w_ref, o_sem.at[1]),
    ]
    for result in results:
        result.start()

    for layer, own, target in ((0, d2, d2_ref), (1, d1, d1_ref)):
        for b in range(3):
            for k in range(1, nj):
                block_copy(layer, k, b).wait_recv()
                for a in range(3):
                    more = got[layer, k, b, a].astype(F32)
                    for c in range(3):
                        own[a, b, c] += more[:, c * half : (c + 1) * half]
            result = pltpu.make_async_copy(
                own.at[:, b], target.at[:, b], o_sem.at[2 + 3 * layer + b]
            )
            result.start()
            results.append(result)
    for result in results:
        result.wait()

    end_moves(moves_two)
    end_moves(moves_one)
    for found in (fields_two, fields_one):
        for _, go, copy, _, _ in found:
            when(go, lambda copy=copy: copy().wait_send())
    sums_end(0, r0)
    sums_end(1, r2)
    sums_end(2, r1)
    for layer in range(2):
        cross(layer).wait_send()
        across(layer).wait_send()
        for k in range(1, nj):
            for b in range(3):
                block_copy(layer, k, b).wait_send()


def hand_over(*refs):
    sources, targets, sems = refs[:4], refs[4:8], refs[8]
    copies = [
        pltpu.make_async_copy(source, target, sems.at[i])
        for i, (source, target) in enumerate(zip(sources, targets))
    ]
    for copy in copies:
        copy.start()
    for copy in copies:
        copy.wait()


def shards(n_t, n_s, features, hidden, cotangent, kernel_one, kernel_two, gains):
    frames, height, width, channels = features.shape
    half = kernel_one.shape[4]
    padded = -(-width // 16) * 16
    if padded < width + 1:
        padded += 16
    q = 2 if n_t % 2 == 0 else 1
    n = n_t * n_s
    nj = n_t // q
    share = channels // n
    cs = channels // (q * n_s)
    rows = frames * height * padded
    lanes = height * padded
    tall = n_s * height

    def wide(field):
        return jnp.pad(field, ((0, 0), (0, 0), (0, padded - width), (0, 0)))

    def stacked(kernel):
        return kernel.transpose(1, 2, 3, 0, 4).reshape(9, 3, channels, half)

    vmem = pl.BlockSpec(memory_space=pltpu.VMEM)
    hbm = pl.BlockSpec(memory_space=pltpu.HBM)
    dma = pltpu.SemaphoreType.DMA
    around = 2 * n_s - 1
    shapes = (
        jax.ShapeDtypeStruct((frames, height * width, half), BF16),
        jax.ShapeDtypeStruct((3, 3, 3, share, half), F32),
        jax.ShapeDtypeStruct((3, 3, 3, share, half), F32),
        jax.ShapeDtypeStruct((2, half), F32),
    )
    passed = pl.BlockSpec(memory_space=pl.ANY)
    results = pl.pallas_call(
        functools.partial(body, (width, n_t, n_s, q)),
        out_shape=shapes,
        in_specs=[vmem, vmem, vmem, hbm, hbm, vmem],
        out_specs=(passed,) * 4,
        scratch_shapes=[
            pltpu.VMEM((frames, height * width, half), BF16),
            pltpu.VMEM((frames, height * width, half), F32),
            pltpu.VMEM((3, 3, 3, share, half), F32),
            pltpu.VMEM((3, 3, 3, share, half), F32),
            pltpu.VMEM((2, half), F32),
            dma((8,)),
            pltpu.VMEM((2, q * frames + 2, tall, padded, half), BF16),
            pltpu.VMEM((2, n_s, frames, height, padded, half), BF16),
            pltpu.VMEM((2, q * frames + 2, tall + 2, padded, 3 * half), BF16),
            pltpu.VMEM((frames, height, padded, half), BF16),
            pltpu.VMEM((2, 9, channels, 3 * half), BF16),
            pltpu.VMEM((2, frames, channels, lanes), BF16),
            pltpu.VMEM((2, q * frames + 2, cs, tall * padded), BF16),
            pltpu.VMEM((2, q * frames + 2, cs, tall * padded), BF16),
            pltpu.VMEM((rows, channels), F32),
            pltpu.VMEM((2, rows, half), BF16),
            pltpu.VMEM((2, rows, half), BF16),
            pltpu.VMEM((8, channels), F32),
            pltpu.VMEM((n, 8, channels), F32),
            pltpu.VMEM((n, 8, half), F32),
            pltpu.VMEM((n, 8, half), F32),
            pltpu.VMEM((2, nj, 3, 3, share, 3 * half), BF16),
            pltpu.VMEM((2, nj, 3, 3, share, 3 * half), BF16),
            pltpu.VMEM((channels, channels), BF16),
            dma((2, 3)),
            dma((2, 2, around)), dma((2, 2, around)),
            dma((2,)), dma((2,)),
            dma((2, 2)), dma((2, 2)),
            dma((2, frames, n_s)), dma((2, frames, n_s)),
            dma((2,)), dma((2,)),
            dma((2, q, n_s)), dma((2, q, n_s)),
            dma((2, q, n_s)), dma((2, n_s)),
            dma((2,)), dma((2,)),
            dma((2, nj, 3)), dma((2, nj, 3)),
            dma((2,)), dma((2,)),
            dma((3, n)), dma((3, n)),
        ],
        compiler_params=pltpu.CompilerParams(
            collective_id=0, has_side_effects=True, vmem_limit_bytes=51 * 1024 * 1024
        ),
    )(wide(features), wide(hidden), wide(cotangent), stacked(kernel_one), stacked(kernel_two), gains)

    grad, delta_one, delta_two, weighted = pl.pallas_call(
        hand_over,
        out_shape=shapes,
        in_specs=[vmem] * 4,
        out_specs=(passed,) * 4,
        scratch_shapes=[dma((4,))],
        compiler_params=pltpu.CompilerParams(vmem_limit_bytes=8 * 1024 * 1024),
    )(*results)

    def unstacked(delta):
        return delta.transpose(3, 0, 1, 2, 4)

    feature_grad = grad.reshape(frames, width, height, half).transpose(0, 2, 1, 3)
    return (feature_grad, unstacked(delta_one), unstacked(delta_two), weighted)


def solution(mesh):
    placed = (
        P(("clip", "tm"), "space", None, None),
        P(("clip", "tm"), "space", None, None),
        P(("clip", "tm"), "space", None, None),
        P(None, None, None, None, "chan"),
        P(None, None, None, None, "chan"),
        P(),
    )
    return jax.shard_map(
        functools.partial(shards, mesh.shape["tm"], mesh.shape["space"]),
        mesh=mesh,
        in_specs=placed,
        out_specs=(
            P(("clip", "tm"), "space", None, "chan"),
            P(("clip", "tm", "space"), None, None, None, "chan"),
            P(("clip", "tm", "space"), None, None, None, "chan"),
            P("clip", "chan"),
        ),
        check_vma=False,
    )
```

```python
import functools

import jax
import jax.numpy as jnp
from jax import lax
from jax.experimental import pallas as pl
from jax.experimental.pallas import tpu as pltpu
from jax.sharding import PartitionSpec as P

GROUPS = 32
EPS = 1e-06
MESH = pl.DeviceIdType.MESH
F32 = jnp.float32
BF16 = jnp.bfloat16


def group_sums(values, per):
    channels = values.shape[1]
    row = lax.broadcasted_iota(jnp.int32, (channels, channels), 0) // per
    col = lax.broadcasted_iota(jnp.int32, (channels, channels), 1) // per
    same = jnp.where(row == col, 1.0, 0.0).astype(F32)
    return jnp.dot(values, same, precision=lax.Precision.HIGHEST, preferred_element_type=F32)


def body(
    sizes,
    f_ref, h_ref, cot_ref, k1_ref, k2_ref, gain_hbm,
    fg_ref, d1_ref, d2_ref, w_ref,
    fg, mixed, d1, d2, weights, gain_ref, o_sem,
    grads, hop, taps, gh, kcat, turned, raw, act, acc, xs, xr, vec, r0, r2, r1, out, got, perm,
    k_sem, gx_s, gx_r, gz_s, gz_r, ge_s, ge_r, gr_s, gr_r, gg_s, gg_r,
    ai_s, ai_r, an_s, an_r, ad_s, ad_r, dl_s, dl_r, xsem_s, xsem_r, ar_s, ar_r,
):
    width, n_t, n_s, q = sizes
    frames, height, padded, channels = cot_ref.shape
    half = channels // 2
    per = channels // GROUPS
    n = n_t * n_s
    nj = n_t // q
    rows = frames * height * padded
    lanes = height * padded
    tall = n_s * height
    share = channels // n
    cs = channels // (q * n_s)
    hc = cs // 2
    t = lax.axis_index("tm")
    s = lax.axis_index("space")
    chan = lax.axis_index("chan")
    partner = 1 - chan
    rank = t * n_s + s
    r = lax.rem(t, q)
    p = t // q
    members = float(frames * height * width * per * n)
    mine = pl.ds(pl.multiple_of(chan * half, half), half)
    theirs = pl.ds(pl.multiple_of(partner * half, half), half)
    own_rows = pl.ds(s * height, height)
    own_frames = pl.ds(r * frames, frames)
    next_frames = pl.ds((r + 1) * frames, frames)
    sibling = {"chan": partner}

    def place(j):
        return {"tm": j // n_s, "space": lax.rem(j, n_s)}

    def peer(k):
        return lax.rem(rank + k, n)

    def each_peer(fn):
        def step(k, carry):
            fn(k)
            return carry

        lax.fori_loop(1, n, step, 0)

    def remote(src, dst, send, recv, device):
        return pltpu.make_async_remote_copy(
            src_ref=src, dst_ref=dst, send_sem=send, recv_sem=recv,
            device_id=device, device_id_type=MESH,
        )

    def kernel_copy(layer, source, c):
        return pltpu.make_async_copy(
            source.at[:, c], kcat.at[layer, :, :, c * half : (c + 1) * half], k_sem.at[layer]
        )

    for c in range(3):
        kernel_copy(0, k2_ref, c).start()
    for c in range(3):
        kernel_copy(1, k1_ref, c).start()

    gain_copy = pltpu.make_async_copy(gain_hbm, gain_ref, o_sem.at[4])
    gain_copy.start()

    barrier = pltpu.get_barrier_semaphore()
    pl.semaphore_signal(barrier, inc=1, device_id=sibling, device_id_type=MESH)
    each_peer(
        lambda k: pl.semaphore_signal(barrier, inc=1, device_id=place(peer(k)), device_id_type=MESH)
    )
    for layer in range(2):
        edge = jnp.zeros((q * frames + 2, 1, padded, 3 * half), BF16)
        taps[layer, :, 0:1] = edge
        taps[layer, :, tall + 1 : tall + 2] = edge

        @pl.when(t == n_t - 1)
        def _(layer=layer):
            def clear(f, carry):
                taps[layer, q * frames + f] = jnp.zeros((tall + 2, padded, 3 * half), BF16)
                return carry

            lax.fori_loop(0, 2, clear, 0)

    pl.semaphore_wait(barrier, n)

    def inside(value, count):
        return (value >= 0) & (value < count)

    def moves(layer, source):
        box = grads.at[layer]
        found = []
        before = jnp.where(r > 0, r, q) * frames
        sent = pl.ds(before, frames)

        def add(kind, go, src, dst, to, come, land, sender, send, recv, ends):
            found.append((
                kind, go, lambda: remote(src, dst, send, recv, to),
                come, None if land is None else lambda: remote(land, land, send, recv, sender),
                None if ends is None else lambda: remote(ends, ends, send, recv, to),
            ))

        for d, (ds, row) in enumerate(((1, height - 1), (-1, 0))):
            back = (s - ds) * height + row
            add(
                "near edge",
                (t > 0) & inside(s + ds, n_s),
                source.at[:, row : row + 1],
                box.at[sent, pl.ds(s * height + row, 1)],
                {"tm": t - 1, "space": s + ds},
                (t + 1 < n_t) & inside(s - ds, n_s),
                box.at[next_frames, pl.ds(back, 1)],
                {"tm": t + 1, "space": s - ds},
                ge_s.at[layer, d], ge_r.at[layer, d], source.at[:, row : row + 1],
            )
        for f in range(frames):
            add(
                f"near {f}", t > 0, source.at[f], box.at[before + f, own_rows], {"tm": t - 1},
                t + 1 < n_t, box.at[(r + 1) * frames + f, own_rows], {"tm": t + 1},
                gz_s.at[layer], gz_r.at[layer, f], source if f == 0 else None,
            )
        for k in sorted((k for k in range(1 - n_s, n_s) if k), key=abs):
            i = k + n_s - 1 if k < 0 else k + n_s - 2
            spans = (("wide", 0, height),)
            if abs(k) == 1:
                spans = (("near x", height - 1, 1), ("wide", 0, height - 1))
                if k < 0:
                    spans = (("near x", 0, 1), ("wide", 1, height - 1))
            for part, (kind, low, count) in enumerate(spans):
                add(
                    kind, inside(s + k, n_s), source.at[:, low : low + count],
                    box.at[own_frames, pl.ds(s * height + low, count)], {"space": s + k},
                    inside(s - k, n_s),
                    box.at[own_frames, pl.ds((s - k) * height + low, count)], {"space": s - k},
                    gx_s.at[layer, i], gx_r.at[layer, part, i], source if part == 0 else None,
                )
        if q > 1:
            for f in range(frames):
                add(
                    f"side {f}", r < q - 1,
                    source.at[f], box.at[r * frames + f, own_rows], {"tm": t + 1},
                    r > 0, box.at[(r - 1) * frames + f, own_rows], {"tm": t - 1},
                    gg_s.at[layer], gg_r.at[layer, f], source if f == 0 else None,
                )
            for k in range(1, n_s):
                to, back = lax.rem(s + k, n_s), lax.rem(s + n_s - k, n_s)
                for f in range(frames):
                    add(
                        f"relay {f}",
                        None, box.at[(q - 1 - r) * frames + f, own_rows], hop.at[layer, k, f],
                        {"space": to},
                        None, hop.at[layer, k] if f == 0 else None, {"space": back},
                        gr_s.at[layer, k - 1], gr_r.at[layer, k - 1],
                        hop.at[layer, k] if f == 0 else None,
                    )
        return found

    def when(predicate, action):
        if predicate is None:
            action()
        else:
            pl.when(predicate)(action)

    def send_moves(found, kinds):
        for kind, go, copy, *_ in found:
            if kind.startswith(kinds):
                when(go, lambda copy=copy: copy().start())

    def take_moves(found, kinds):
        for kind, _, _, come, copy, _ in found:
            if kind.startswith(kinds) and copy is not None:
                when(come, lambda copy=copy: copy().wait_recv())

    def end_moves(found):
        for _, go, _, _, _, copy in found:
            if copy is not None:
                when(go, lambda copy=copy: copy().wait_send())

    def set_rows(to_r, to_s):
        start = (to_r * n_s + to_s) * cs + chan * hc
        return pl.ds(pl.multiple_of(start, hc), hc)

    my_half = pl.ds(pl.multiple_of(chan * hc, hc), hc)

    def strip(at):
        return pl.ds(pl.multiple_of(at * lanes, lanes), lanes)

    def field_moves(layer):
        found = []
        for dr in range(q):
            for k in range(n_s):
                if dr == 0 and k == 0:
                    continue
                to_r, to_s = lax.rem(r + dr, q), lax.rem(s + k, n_s)
                src = turned.at[layer, :, set_rows(to_r, to_s)]
                dst = raw.at[layer, pl.ds(2 + r * frames, frames), my_half, strip(s)]
                found.append((None, functools.partial(
                    remote, src, dst, ai_s.at[layer], ai_r.at[layer],
                    {"tm": p * q + to_r, "space": to_s},
                )))
        for to_r in range(q):
            for k in range(n_s):
                to_s = lax.rem(s + k, n_s)
                src = turned.at[layer, frames - 2 : frames, set_rows(to_r, to_s)]
                dst = raw.at[layer, 0:2, my_half, strip(s)]
                found.append(((r == q - 1) & (p + 1 < nj), functools.partial(
                    remote, src, dst, an_s.at[layer], an_r.at[layer],
                    {"tm": (p + 1) * q + to_r, "space": to_s},
                )))
        return found

    def send_fields(found):
        for go, copy in found:
            when(go, lambda copy=copy: copy().start())

    def fields_like(layer, count, first, send, recv):
        cells = turned.at[layer, first:frames, 0 : count * hc]
        return remote(cells, cells, send.at[layer], recv.at[layer], sibling)

    def take_fields(layer):
        if q * n_s > 1:
            fields_like(layer, q * n_s - 1, 0, ai_s, ai_r).wait_recv()

        @pl.when(p > 0)
        def _():
            fields_like(layer, n_s, frames - 2, an_s, an_r).wait_recv()

    def end_fields(layer):
        if q * n_s > 1:
            fields_like(layer, q * n_s - 1, 0, ai_s, ai_r).wait_send()

        @pl.when((r == q - 1) & (p + 1 < nj))
        def _():
            fields_like(layer, q * n_s, frames - 2, an_s, an_r).wait_send()

    def across(layer):
        half_set = raw.at[layer, :, my_half]
        return remote(half_set, half_set, ad_s.at[layer], ad_r.at[layer], sibling)

    def across_land(layer):
        other = raw.at[layer, :, pl.ds(pl.multiple_of(partner * hc, hc), hc)]
        return remote(other, other, ad_s.at[layer], ad_r.at[layer], sibling)

    def sums_copy(layer, buf, device, part):
        return remote(part, part, ar_s.at[layer], ar_r.at[layer], device)

    def sums_start(layer, buf, values):
        buf[rank] = values
        each_peer(lambda k: sums_copy(layer, buf, place(peer(k)), buf.at[rank]).start())

    def sums_finish(layer, buf):
        sums_copy(layer, buf, sibling, buf.at[0 : n - 1]).wait_recv()
        return jnp.sum(buf[...], axis=0)

    def sums_end(layer, buf):
        sums_copy(layer, buf, sibling, buf.at[0 : n - 1]).wait_send()

    def block_copy(layer, k, b):
        to = lax.rem(p + k, nj)
        return remote(
            out.at[layer, to, b], got.at[layer, k, b], dl_s.at[layer, k - 1], dl_r.at[layer, k - 1, b],
            {"tm": to * q + r},
        )

    def cross(layer):
        return remote(xs.at[layer], xr.at[layer], xsem_s.at[layer], xsem_r.at[layer], sibling)

    column = lax.rem(lax.broadcasted_iota(jnp.int32, (rows, 1), 0), padded)
    real = column < width

    def spread(layer, f, row, source):
        count = source.shape[0]
        cells = source.reshape(count * padded, half).astype(F32)
        size = count * padded
        ahead = pltpu.roll(cells, size - 1, 0)
        behind = pltpu.roll(cells, 1, 0)
        for c, value in enumerate((ahead, cells, behind)):
            taps[layer, f, pl.ds(row + 1, count), :, c * half : (c + 1) * half] = value.astype(
                BF16
            ).reshape(count, padded, half)

    def fill(layer, f, row, count):
        spread(layer, f, row, grads[layer, f, pl.ds(row, count)])

    def fill_rows(layer, f):
        fill(layer, f, s * height, height)
        for row, ok in ((s * height - 1, s > 0), ((s + 1) * height, s + 1 < n_s)):
            pl.when(ok)(functools.partial(fill, layer, f, row, 1))

    def land(layer):
        take_moves(moves_of[layer], ("near edge",))
        for f in range(frames):
            take_moves(moves_of[layer], (f"near {f}", f"side {f}"))
            if layer == 1 or f == 0:
                send_moves(moves_of[layer], (f"relay {f}",))
            pl.when(t + 1 < n_t)(functools.partial(fill_rows, layer, (r + 1) * frames + f))

    def fill_own(layer):
        take_moves(moves_of[layer], ("near x",))
        for f in range(frames):
            fill_rows(layer, r * frames + f)

    def fill_rest(layer):
        for k in range(1, n_s):
            back = lax.rem(s + n_s - k, n_s)
            for f in range(frames):
                fill(layer, r * frames + f, back * height, height)
                if q > 1:
                    mate = (q - 1 - r) * frames + f
                    spread(layer, mate, back * height, hop[layer, k, f])
        if q > 1:
            @pl.when(r > 0)
            def _():
                for f in range(frames):
                    fill(layer, f, s * height, height)

    def conv(layer, source, near):
        if near:
            pltpu.make_async_copy(kcat.at[layer], kcat.at[layer], k_sem.at[layer]).wait()
        for f in range(frames):
            total = None
            for ab in range(9):
                a, b = ab // 3, ab % 3
                if (2 - a + f < frames) != near:
                    continue
                left = taps[
                    layer, r * frames + (2 - a + f), pl.ds(s * height + (2 - b), height)
                ].reshape(lanes, 3 * half)
                term = lax.dot_general(
                    left, kcat[layer, ab], (((1,), (1,)), ((), ())), preferred_element_type=F32
                )
                total = term if total is None else total + term
            if total is None:
                continue
            if near:
                acc[f * lanes : (f + 1) * lanes] = total
            else:
                acc[f * lanes : (f + 1) * lanes] += total
        if not near:
            xs[layer] = acc[:, theirs].astype(BF16)
            cross(layer).start()

    def norm_back(field_ref, base, layer):
        cross(layer).wait_recv()
        upstream = acc[:, mine] + xr[layer].astype(F32)
        field = field_ref[:, :, :, mine].reshape(rows, half).astype(F32)
        scale = vec[base + 1 : base + 2, mine]
        gain = vec[base + 2 : base + 3, mine]
        centred = (field - vec[base : base + 1, mine]) * scale
        scaled = centred * gain
        gate = jax.nn.sigmoid(scaled)
        slope = jnp.where(real, upstream * gate * (1.0 + scaled * (1.0 - gate)), 0.0)
        acc[:, mine] = slope
        parts = [
            jnp.sum(slope, axis=0, keepdims=True),
            jnp.sum(slope * centred, axis=0, keepdims=True),
            jnp.zeros((6, half), F32),
        ]
        sums_start(layer + 1, (r2, r1)[layer], jnp.concatenate(parts, axis=0))

    def norm_end(field_ref, base, layer, w_row):
        totals = sums_finish(layer + 1, (r2, r1)[layer])
        weights[w_row : w_row + 1] = totals[1:2]
        scale = vec[base + 1 : base + 2, mine]
        gain = vec[base + 2 : base + 3, mine]
        means = group_sums(totals * gain, per) / members
        field = field_ref[:, :, :, mine].reshape(rows, half).astype(F32)
        centred = (field - vec[base : base + 1, mine]) * scale
        grad = scale * (acc[:, mine] * gain - means[0:1] - centred * means[1:2])
        return jnp.where(real, grad, 0.0)

    def turn(field_ref, layer):
        for f in range(frames):
            cells = field_ref[f].reshape(lanes, channels)
            flat = lax.dot_general(
                perm[...], cells, (((1,), (1,)), ((), ())), preferred_element_type=F32
            ).astype(BF16)
            turned[layer, f] = flat
        raw[layer, pl.ds(2 + r * frames, frames), my_half, strip(s)] = turned[layer, :, set_rows(r, s)]

    def activate(layer, base):
        pick = perm[pl.ds(pl.multiple_of((r * n_s + s) * cs, cs), cs)].astype(F32)
        cols = lax.dot_general(
            pick, vec[...], (((1,), (1,)), ((), ())),
            precision=lax.Precision.HIGHEST, preferred_element_type=F32,
        )
        mean, scale, gain = (cols[:, base + i : base + i + 1] for i in range(3))
        spot = lax.rem(lax.broadcasted_iota(jnp.int32, (1, tall * padded), 1), padded)

        def step(f, carry):
            field = raw[layer, f].astype(F32)
            scaled = (field - mean) * scale * gain
            keep = (spot < width) & ((f >= 2) | (p > 0))
            active = jnp.where(keep, scaled * jax.nn.sigmoid(scaled), 0.0)
            act[layer, f] = active.astype(BF16)
            return carry

        lax.fori_loop(0, q * frames + 2, step, 0)

    def delta(layer, own):
        for b in range(3):
            product = None
            for f in range(q * frames):
                left = act[layer, f : f + 3].reshape(3 * cs, tall * padded)
                right = taps[layer, f, 2 - b : 2 - b + tall].reshape(tall * padded, 3 * half)
                term = jnp.dot(left, right, preferred_element_type=F32)
                product = term if product is None else product + term
            small = product.astype(BF16)
            for j in range(nj):
                for a in range(3):
                    low = a * cs + j * share
                    out[layer, j, b, a] = small[low : low + share]

                @pl.when(p == j)
                def _(j=j):
                    for a in range(3):
                        low = a * cs + j * share
                        for c in range(3):
                            own[a, b, c] = product[
                                low : low + share, c * half : (c + 1) * half
                            ]

            for k in range(1, nj):
                block_copy(layer, k, b).start()

    moves_of = (moves(0, cot_ref.at[:, :, :, mine]), moves(1, gh))
    send_moves(moves_of[0], ("near", "side"))
    send_moves(moves_of[0], ("wide",))
    grads[0, own_frames, own_rows] = cot_ref[:, :, :, mine]

    field_one = f_ref[...].reshape(rows, channels).astype(F32)
    field_two = h_ref[...].reshape(rows, channels).astype(F32)
    parts = [
        jnp.sum(field_one, axis=0, keepdims=True),
        jnp.sum(field_one * field_one, axis=0, keepdims=True),
        jnp.sum(field_two, axis=0, keepdims=True),
        jnp.sum(field_two * field_two, axis=0, keepdims=True),
        jnp.zeros((4, channels), F32),
    ]
    sums_start(0, r0, jnp.concatenate(parts, axis=0))

    place_row = lax.broadcasted_iota(jnp.int32, (channels, channels), 0)
    place_col = lax.broadcasted_iota(jnp.int32, (channels, channels), 1)
    element = lax.rem(place_row, share)
    block = lax.rem(place_row // share, nj)
    which = place_row // (share * nj)
    wanted = ((block * q + which // n_s) * n_s + lax.rem(which, n_s)) * share + element
    perm[...] = jnp.where(place_col == wanted, 1.0, 0.0).astype(BF16)

    fields_two = field_moves(0)
    fields_one = field_moves(1)

    turn(h_ref, 0)
    turn(f_ref, 1)

    fill_own(0)
    conv(0, k2_ref, True)
    land(0)
    send_fields(fields_two)
    conv(0, k2_ref, False)
    gain_copy.wait()

    totals = group_sums(sums_finish(0, r0), per) / members
    mean_one, mean_two = totals[0:1], totals[2:3]
    vec[0:1] = mean_one
    vec[1:2] = lax.rsqrt(totals[1:2] - mean_one * mean_one + EPS)
    vec[2:3] = gain_ref[0:1]
    vec[3:4] = mean_two
    vec[4:5] = lax.rsqrt(totals[3:4] - mean_two * mean_two + EPS)
    vec[5:6] = gain_ref[1:2]
    vec[6:8] = jnp.zeros((2, channels), F32)

    norm_back(h_ref, 3, 0)
    for f in range(1, frames):
        send_moves(moves_of[0], (f"relay {f}",))
    send_fields(fields_one)
    gh[...] = norm_end(h_ref, 3, 0, 1).astype(BF16).reshape(frames, height, padded, half)
    send_moves(moves_of[1], ("near", "side"))
    send_moves(moves_of[1], ("wide",))
    grads[1, own_frames, own_rows] = gh[...]

    take_fields(0)
    across(0).start()
    take_moves(moves_of[0], ("wide", "relay"))
    fill_rest(0)
    across_land(0).wait_recv()
    activate(0, 3)
    delta(0, d2)
    fill_own(1)
    conv(1, k1_ref, True)
    land(1)
    conv(1, k1_ref, False)
    take_fields(1)
    across(1).start()
    norm_back(f_ref, 0, 1)
    across_land(1).wait_recv()
    activate(1, 0)
    take_moves(moves_of[1], ("wide", "relay"))
    fill_rest(1)
    delta(1, d1)
    grad = norm_end(f_ref, 0, 1, 0)
    total = cot_ref[:, :, :, mine].reshape(rows, half).astype(F32) + grad
    for f in range(frames):
        for h in range(height):
            at = (f * height + h) * padded
            mixed[f, pl.ds(h, width, stride=height)] = total[at : at + width]
    fg[...] = mixed[...].astype(BF16)
    results = [
        pltpu.make_async_copy(fg, fg_ref, o_sem.at[0]),
        pltpu.make_async_copy(weights, w_ref, o_sem.at[1]),
    ]
    for result in results:
        result.start()

    for layer, own, target in ((0, d2, d2_ref), (1, d1, d1_ref)):
        for b in range(3):
            for k in range(1, nj):
                block_copy(layer, k, b).wait_recv()
                for a in range(3):
                    more = got[layer, k, b, a].astype(F32)
                    for c in range(3):
                        own[a, b, c] += more[:, c * half : (c + 1) * half]
            result = pltpu.make_async_copy(
                own.at[:, b], target.at[:, b], o_sem.at[2 + layer]
            )
            result.start()
        results.append(pltpu.make_async_copy(own, target, o_sem.at[2 + layer]))
    for result in results:
        result.wait()

    end_moves(moves_of[0])
    end_moves(moves_of[1])
    end_fields(0)
    end_fields(1)
    sums_end(0, r0)
    sums_end(1, r2)
    sums_end(2, r1)
    for layer in range(2):
        cross(layer).wait_send()
        across(layer).wait_send()
        for k in range(1, nj):
            whole = out.at[layer, 0]
            remote(whole, whole, dl_s.at[layer, k - 1], dl_r.at[layer, k - 1, 0], sibling).wait_send()


def hand_over(*refs):
    sources, targets, sems = refs[:4], refs[4:8], refs[8]
    copies = [
        pltpu.make_async_copy(source, target, sems.at[i])
        for i, (source, target) in enumerate(zip(sources, targets))
    ]
    for copy in copies:
        copy.start()
    for copy in copies:
        copy.wait()


def shards(n_t, n_s, features, hidden, cotangent, kernel_one, kernel_two, gains):
    frames, height, width, channels = features.shape
    half = kernel_one.shape[4]
    padded = -(-width // 16) * 16
    if padded < width + 1:
        padded += 16
    q = 2 if n_t % 2 == 0 else 1
    n = n_t * n_s
    nj = n_t // q
    share = channels // n
    cs = channels // (q * n_s)
    rows = frames * height * padded
    lanes = height * padded
    tall = n_s * height

    def wide(field):
        return jnp.pad(field, ((0, 0), (0, 0), (0, padded - width), (0, 0)))

    def stacked(kernel):
        return kernel.transpose(1, 2, 3, 0, 4).reshape(9, 3, channels, half)

    vmem = pl.BlockSpec(memory_space=pltpu.VMEM)
    hbm = pl.BlockSpec(memory_space=pltpu.HBM)
    dma = pltpu.SemaphoreType.DMA
    shapes = (
        jax.ShapeDtypeStruct((frames, height * width, half), BF16),
        jax.ShapeDtypeStruct((3, 3, 3, share, half), F32),
        jax.ShapeDtypeStruct((3, 3, 3, share, half), F32),
        jax.ShapeDtypeStruct((2, half), F32),
    )
    passed = pl.BlockSpec(memory_space=pl.ANY)
    results = pl.pallas_call(
        functools.partial(body, (width, n_t, n_s, q)),
        out_shape=shapes,
        in_specs=[vmem, vmem, vmem, hbm, hbm, hbm],
        out_specs=(passed,) * 4,
        scratch_shapes=[
            pltpu.VMEM((frames, height * width, half), BF16),
            pltpu.VMEM((frames, height * width, half), F32),
            pltpu.VMEM((3, 3, 3, share, half), F32),
            pltpu.VMEM((3, 3, 3, share, half), F32),
            pltpu.VMEM((2, half), F32),
            pltpu.VMEM((2, channels), F32),
            dma((5,)),
            pltpu.VMEM((2, q * frames + 2, tall, padded, half), BF16),
            pltpu.VMEM((2, n_s, frames, height, padded, half), BF16),
            pltpu.VMEM((2, q * frames + 2, tall + 2, padded, 3 * half), BF16),
            pltpu.VMEM((frames, height, padded, half), BF16),
            pltpu.VMEM((2, 9, channels, 3 * half), BF16),
            pltpu.VMEM((2, frames, channels, lanes), BF16),
            pltpu.VMEM((2, q * frames + 2, cs, tall * padded), BF16),
            pltpu.VMEM((2, q * frames + 2, cs, tall * padded), BF16),
            pltpu.VMEM((rows, channels), F32),
            pltpu.VMEM((2, rows, half), BF16),
            pltpu.VMEM((2, rows, half), BF16),
            pltpu.VMEM((8, channels), F32),
            pltpu.VMEM((n, 8, channels), F32),
            pltpu.VMEM((n, 8, half), F32),
            pltpu.VMEM((n, 8, half), F32),
            pltpu.VMEM((2, nj, 3, 3, share, 3 * half), BF16),
            pltpu.VMEM((2, nj, 3, 3, share, 3 * half), BF16),
            pltpu.VMEM((channels, channels), BF16),
            dma((2,)),
            dma((2, 2 * n_s - 2)), dma((2, 2, 2 * n_s - 2)),
            dma((2,)), dma((2, frames)),
            dma((2, 2)), dma((2, 2)),
            dma((2, n_s - 1)), dma((2, n_s - 1)),
            dma((2,)), dma((2, frames)),
            dma((2,)), dma((2,)),
            dma((2,)), dma((2,)),
            dma((2,)), dma((2,)),
            dma((2, nj - 1)), dma((2, nj - 1, 3)),
            dma((2,)), dma((2,)),
            dma((3,)), dma((3,)),
        ],
        compiler_params=pltpu.CompilerParams(
            collective_id=0, has_side_effects=True, vmem_limit_bytes=51 * 1024 * 1024
        ),
    )(wide(features), wide(hidden), wide(cotangent), stacked(kernel_one), stacked(kernel_two), gains)

    grad, delta_one, delta_two, weighted = pl.pallas_call(
        hand_over,
        out_shape=shapes,
        in_specs=[vmem] * 4,
        out_specs=(passed,) * 4,
        scratch_shapes=[dma((4,))],
        compiler_params=pltpu.CompilerParams(vmem_limit_bytes=8 * 1024 * 1024),
    )(*results)

    def unstacked(delta):
        return delta.transpose(3, 0, 1, 2, 4)

    feature_grad = grad.reshape(frames, width, height, half).transpose(0, 2, 1, 3)
    return (feature_grad, unstacked(delta_one), unstacked(delta_two), weighted)


def solution(mesh):
    placed = (
        P(("clip", "tm"), "space", None, None),
        P(("clip", "tm"), "space", None, None),
        P(("clip", "tm"), "space", None, None),
        P(None, None, None, None, "chan"),
        P(None, None, None, None, "chan"),
        P(),
    )
    return jax.shard_map(
        functools.partial(shards, mesh.shape["tm"], mesh.shape["space"]),
        mesh=mesh,
        in_specs=placed,
        out_specs=(
            P(("clip", "tm"), "space", None, "chan"),
            P(("clip", "tm", "space"), None, None, None, "chan"),
            P(("clip", "tm", "space"), None, None, None, "chan"),
            P("clip", "chan"),
        ),
        check_vma=False,
    )
```

```python
import functools

import jax
import jax.numpy as jnp
from jax import lax
from jax.experimental import pallas as pl
from jax.experimental.pallas import tpu as pltpu
from jax.sharding import PartitionSpec as P

GROUPS = 32
SOON = 2
EPS = 1e-06
MESH = pl.DeviceIdType.MESH
F32 = jnp.float32
BF16 = jnp.bfloat16


def group_sums(values, per):
    channels = values.shape[1]
    row = lax.broadcasted_iota(jnp.int32, (channels, channels), 0) // per
    col = lax.broadcasted_iota(jnp.int32, (channels, channels), 1) // per
    same = jnp.where(row == col, 1.0, 0.0).astype(F32)
    return jnp.dot(values, same, precision=lax.Precision.HIGHEST, preferred_element_type=F32)


def body(
    sizes,
    f_ref, h_ref, cot_ref, k1_ref, k2_ref, gain_hbm,
    fg_ref, d1_ref, d2_ref, w_ref,
    fg, mixed, d1, d2, weights, gain_ref, o_sem,
    grads, hop, taps, gh, kcat, turned, raw, act, acc, xs, xr, vec, r0, r2, r1, out, got, perm,
    k_sem, gx_s, gx_r, gz_s, gz_r, ge_s, ge_r, gr_s, gr_r, gg_s, gg_r,
    ai_s, ai_r, an_s, an_r, ad_s, ad_r, dl_s, dl_r, xsem_s, xsem_r, ar_s, ar_r,
):
    width, n_t, n_s, q = sizes
    frames, height, padded, channels = cot_ref.shape
    half = channels // 2
    per = channels // GROUPS
    n = n_t * n_s
    nj = n_t // q
    rows = frames * height * padded
    lanes = height * padded
    tall = n_s * height
    share = channels // n
    cs = channels // (q * n_s)
    hc = cs // 2
    t = lax.axis_index("tm")
    s = lax.axis_index("space")
    chan = lax.axis_index("chan")
    partner = 1 - chan
    rank = t * n_s + s
    r = lax.rem(t, q)
    p = t // q
    held = (r == q - 1) & (p > 0)
    members = float(frames * height * width * per * n)
    mine = pl.ds(pl.multiple_of(chan * half, half), half)
    theirs = pl.ds(pl.multiple_of(partner * half, half), half)
    own_rows = pl.ds(s * height, height)
    own_frames = pl.ds(r * frames, frames)
    next_frames = pl.ds((r + 1) * frames, frames)
    sibling = {"chan": partner}

    def place(j):
        return {"tm": j // n_s, "space": lax.rem(j, n_s)}

    def peer(k):
        return lax.rem(rank + k, n)

    def each_peer(fn):
        def step(k, carry):
            fn(k)
            return carry

        lax.fori_loop(1, n, step, 0)

    def remote(src, dst, send, recv, device):
        return pltpu.make_async_remote_copy(
            src_ref=src, dst_ref=dst, send_sem=send, recv_sem=recv,
            device_id=device, device_id_type=MESH,
        )

    def kernel_copy(layer, source, c):
        return pltpu.make_async_copy(
            source.at[:, c], kcat.at[layer, :, :, c * half : (c + 1) * half], k_sem.at[layer]
        )

    for c in range(3):
        kernel_copy(0, k2_ref, c).start()
    for c in range(3):
        kernel_copy(1, k1_ref, c).start()

    gain_copy = pltpu.make_async_copy(gain_hbm, gain_ref, o_sem.at[4])
    gain_copy.start()

    barrier = pltpu.get_barrier_semaphore()
    pl.semaphore_signal(barrier, inc=1, device_id=sibling, device_id_type=MESH)
    each_peer(
        lambda k: pl.semaphore_signal(barrier, inc=1, device_id=place(peer(k)), device_id_type=MESH)
    )
    for layer in range(2):
        edge = jnp.zeros((q * frames + 2, 1, padded, 3 * half), BF16)
        taps[layer, :, 0:1] = edge
        taps[layer, :, tall + 1 : tall + 2] = edge

        @pl.when(t == n_t - 1)
        def _(layer=layer):
            def clear(f, carry):
                taps[layer, q * frames + f] = jnp.zeros((tall + 2, padded, 3 * half), BF16)
                return carry

            lax.fori_loop(0, 2, clear, 0)

    pl.semaphore_wait(barrier, n)

    def inside(value, count):
        return (value >= 0) & (value < count)

    def moves(layer, source):
        box = grads.at[layer]
        found = []
        before = jnp.where(r > 0, r, q) * frames
        sent = pl.ds(before, frames)

        def add(kind, go, src, dst, to, come, land, sender, send, recv, ends):
            found.append((
                kind, go, lambda: remote(src, dst, send, recv, to),
                come, None if land is None else lambda: remote(land, land, send, recv, sender),
                None if ends is None else lambda: remote(ends, ends, send, recv, to),
            ))

        for d, (ds, row) in enumerate(((1, height - 1), (-1, 0))):
            back = (s - ds) * height + row
            add(
                "near edge",
                (t > 0) & inside(s + ds, n_s),
                source.at[:, row : row + 1],
                box.at[sent, pl.ds(s * height + row, 1)],
                {"tm": t - 1, "space": s + ds},
                (t + 1 < n_t) & inside(s - ds, n_s),
                box.at[next_frames, pl.ds(back, 1)],
                {"tm": t + 1, "space": s - ds},
                ge_s.at[layer, d], ge_r.at[layer, d], source.at[:, row : row + 1],
            )
        for f in range(frames):
            add(
                f"near {f}", t > 0, source.at[f], box.at[before + f, own_rows], {"tm": t - 1},
                t + 1 < n_t, box.at[(r + 1) * frames + f, own_rows], {"tm": t + 1},
                gz_s.at[layer], gz_r.at[layer, f], source if f == 0 else None,
            )
        for k in sorted((k for k in range(1 - n_s, n_s) if k), key=abs):
            i = k + n_s - 1 if k < 0 else k + n_s - 2
            spans = (("wide", 0, height),)
            if abs(k) == 1:
                spans = (("near x", height - 1, 1), ("wide", 0, height - 1))
                if k < 0:
                    spans = (("near x", 0, 1), ("wide", 1, height - 1))
            for part, (kind, low, count) in enumerate(spans):
                add(
                    kind, inside(s + k, n_s), source.at[:, low : low + count],
                    box.at[own_frames, pl.ds(s * height + low, count)], {"space": s + k},
                    inside(s - k, n_s),
                    box.at[own_frames, pl.ds((s - k) * height + low, count)], {"space": s - k},
                    gx_s.at[layer, i], gx_r.at[layer, part, i], source if part == 0 else None,
                )
        if q > 1:
            for f in range(frames):
                add(
                    f"side {f}", r < q - 1,
                    source.at[f], box.at[r * frames + f, own_rows], {"tm": t + 1},
                    r > 0, box.at[(r - 1) * frames + f, own_rows], {"tm": t - 1},
                    gg_s.at[layer], gg_r.at[layer, f], source if f == 0 else None,
                )
            for k in range(1, n_s):
                to, back = lax.rem(s + k, n_s), lax.rem(s + n_s - k, n_s)
                for f in range(frames):
                    add(
                        f"relay {f}",
                        None, box.at[(q - 1 - r) * frames + f, own_rows], hop.at[layer, k, f],
                        {"space": to},
                        None, hop.at[layer, k] if f == 0 else None, {"space": back},
                        gr_s.at[layer, k - 1], gr_r.at[layer, k - 1],
                        hop.at[layer, k] if f == 0 else None,
                    )
        return found

    def when(predicate, action):
        if predicate is None:
            action()
        else:
            pl.when(predicate)(action)

    def send_moves(found, kinds):
        for kind, go, copy, *_ in found:
            if kind.startswith(kinds):
                when(go, lambda copy=copy: copy().start())

    def take_moves(found, kinds):
        for kind, _, _, come, copy, _ in found:
            if kind.startswith(kinds) and copy is not None:
                when(come, lambda copy=copy: copy().wait_recv())

    def end_moves(found):
        for _, go, _, _, _, copy in found:
            if copy is not None:
                when(go, lambda copy=copy: copy().wait_send())

    def set_rows(to_r, to_s):
        start = (to_r * n_s + to_s) * cs + chan * hc
        return pl.ds(pl.multiple_of(start, hc), hc)

    my_half = pl.ds(pl.multiple_of(chan * hc, hc), hc)

    def strip(at):
        return pl.ds(pl.multiple_of(at * lanes, lanes), lanes)

    def field_moves(layer):
        found = []
        for dr in range(q):
            for k in range(n_s):
                if dr == 0 and k == 0:
                    continue
                to_r, to_s = lax.rem(r + dr, q), lax.rem(s + k, n_s)
                src = turned.at[layer, :, set_rows(to_r, to_s)]
                dst = raw.at[layer, pl.ds(2 + r * frames, frames), my_half, strip(s)]
                found.append((None, functools.partial(
                    remote, src, dst, ai_s.at[layer], ai_r.at[layer],
                    {"tm": p * q + to_r, "space": to_s},
                )))
        for to_r in range(q):
            for k in range(n_s):
                to_s = lax.rem(s + k, n_s)
                src = turned.at[layer, frames - 2 : frames, set_rows(to_r, to_s)]
                dst = raw.at[layer, 0:2, my_half, strip(s)]
                found.append(((r == q - 1) & (p + 1 < nj), functools.partial(
                    remote, src, dst, an_s.at[layer], an_r.at[layer],
                    {"tm": (p + 1) * q + to_r, "space": to_s},
                )))
        return found

    def send_fields(found):
        for go, copy in found:
            when(go, lambda copy=copy: copy().start())

    def fields_like(layer, count, first, send, recv):
        cells = turned.at[layer, first:frames, 0 : count * hc]
        return remote(cells, cells, send.at[layer], recv.at[layer], sibling)

    def take_fields(layer):
        if q * n_s > 1:
            fields_like(layer, q * n_s - 1, 0, ai_s, ai_r).wait_recv()

        @pl.when(p > 0)
        def _():
            fields_like(layer, n_s, frames - 2, an_s, an_r).wait_recv()

    def end_fields(layer):
        if q * n_s > 1:
            fields_like(layer, q * n_s - 1, 0, ai_s, ai_r).wait_send()

        @pl.when((r == q - 1) & (p + 1 < nj))
        def _():
            fields_like(layer, q * n_s, frames - 2, an_s, an_r).wait_send()

    def across(layer):
        half_set = raw.at[layer, :, my_half]
        return remote(half_set, half_set, ad_s.at[layer], ad_r.at[layer], sibling)

    def across_land(layer):
        other = raw.at[layer, :, pl.ds(pl.multiple_of(partner * hc, hc), hc)]
        return remote(other, other, ad_s.at[layer], ad_r.at[layer], sibling)

    def sums_copy(layer, buf, device, part):
        return remote(part, part, ar_s.at[layer], ar_r.at[layer], device)

    def sums_start(layer, buf, values):
        buf[rank] = values
        each_peer(lambda k: sums_copy(layer, buf, place(peer(k)), buf.at[rank]).start())

    def sums_finish(layer, buf):
        sums_copy(layer, buf, sibling, buf.at[0 : n - 1]).wait_recv()
        return jnp.sum(buf[...], axis=0)

    def sums_end(layer, buf):
        sums_copy(layer, buf, sibling, buf.at[0 : n - 1]).wait_send()

    def block_copy(layer, k, b):
        to = lax.rem(p + k, nj)
        return remote(
            out.at[layer, to, b], got.at[layer, k, b], dl_s.at[layer, k - 1], dl_r.at[layer, k - 1, b],
            {"tm": to * q + r},
        )

    def cross(layer):
        return remote(xs.at[layer], xr.at[layer], xsem_s.at[layer], xsem_r.at[layer], sibling)

    column = lax.rem(lax.broadcasted_iota(jnp.int32, (rows, 1), 0), padded)
    real = column < width

    def spread(layer, f, row, source):
        count = source.shape[0]
        cells = source.reshape(count * padded, half).astype(F32)
        size = count * padded
        ahead = pltpu.roll(cells, size - 1, 0)
        behind = pltpu.roll(cells, 1, 0)
        for c, value in enumerate((ahead, cells, behind)):
            taps[layer, f, pl.ds(row + 1, count), :, c * half : (c + 1) * half] = value.astype(
                BF16
            ).reshape(count, padded, half)

    def fill(layer, f, row, count):
        spread(layer, f, row, grads[layer, f, pl.ds(row, count)])

    def fill_rows(layer, f):
        fill(layer, f, s * height, height)
        for row, ok in ((s * height - 1, s > 0), ((s + 1) * height, s + 1 < n_s)):
            pl.when(ok)(functools.partial(fill, layer, f, row, 1))

    def land(layer):
        take_moves(moves_of[layer], ("near edge",))
        for f in range(frames):
            take_moves(moves_of[layer], (f"near {f}", f"side {f}"))
            if layer == 1 or f == 0:
                send_moves(moves_of[layer], (f"relay {f}",))
            pl.when(t + 1 < n_t)(functools.partial(fill_rows, layer, (r + 1) * frames + f))

    def fill_own(layer):
        take_moves(moves_of[layer], ("near x",))
        for f in range(frames):
            fill_rows(layer, r * frames + f)

    def fill_rest(layer):
        for k in range(1, n_s):
            back = lax.rem(s + n_s - k, n_s)
            for f in range(frames):
                fill(layer, r * frames + f, back * height, height)
                if q > 1:
                    mate = (q - 1 - r) * frames + f
                    spread(layer, mate, back * height, hop[layer, k, f])
        if q > 1:
            @pl.when(r > 0)
            def _():
                for f in range(frames):
                    fill(layer, f, s * height, height)

    def conv(layer, source, near):
        if near:
            pltpu.make_async_copy(kcat.at[layer], kcat.at[layer], k_sem.at[layer]).wait()
        for f in range(frames):
            total = None
            for ab in range(9):
                a, b = ab // 3, ab % 3
                if (2 - a + f < frames) != near:
                    continue
                left = taps[
                    layer, r * frames + (2 - a + f), pl.ds(s * height + (2 - b), height)
                ].reshape(lanes, 3 * half)
                term = lax.dot_general(
                    left, kcat[layer, ab], (((1,), (1,)), ((), ())), preferred_element_type=F32
                )
                total = term if total is None else total + term
            if total is None:
                continue
            if near:
                acc[f * lanes : (f + 1) * lanes] = total
            else:
                acc[f * lanes : (f + 1) * lanes] += total
        if not near:
            xs[layer] = acc[:, theirs].astype(BF16)
            cross(layer).start()

    def norm_back(field_ref, base, layer):
        cross(layer).wait_recv()
        upstream = acc[:, mine] + xr[layer].astype(F32)
        field = field_ref[:, :, :, mine].reshape(rows, half).astype(F32)
        scale = vec[base + 1 : base + 2, mine]
        gain = vec[base + 2 : base + 3, mine]
        centred = (field - vec[base : base + 1, mine]) * scale
        scaled = centred * gain
        gate = jax.nn.sigmoid(scaled)
        slope = jnp.where(real, upstream * gate * (1.0 + scaled * (1.0 - gate)), 0.0)
        acc[:, mine] = slope
        parts = [
            jnp.sum(slope, axis=0, keepdims=True),
            jnp.sum(slope * centred, axis=0, keepdims=True),
            jnp.zeros((6, half), F32),
        ]
        sums_start(layer + 1, (r2, r1)[layer], jnp.concatenate(parts, axis=0))

    def norm_end(field_ref, base, layer, w_row):
        totals = sums_finish(layer + 1, (r2, r1)[layer])
        weights[w_row : w_row + 1] = totals[1:2]
        scale = vec[base + 1 : base + 2, mine]
        gain = vec[base + 2 : base + 3, mine]
        means = group_sums(totals * gain, per) / members
        field = field_ref[:, :, :, mine].reshape(rows, half).astype(F32)
        centred = (field - vec[base : base + 1, mine]) * scale
        grad = scale * (acc[:, mine] * gain - means[0:1] - centred * means[1:2])
        return jnp.where(real, grad, 0.0)

    def turn(field_ref, layer):
        for f in range(frames):
            cells = field_ref[f].reshape(lanes, channels)
            flat = lax.dot_general(
                perm[...], cells, (((1,), (1,)), ((), ())), preferred_element_type=F32
            ).astype(BF16)
            turned[layer, f] = flat
        raw[layer, pl.ds(2 + r * frames, frames), my_half, strip(s)] = turned[layer, :, set_rows(r, s)]

    def activate(layer, base):
        pick = perm[pl.ds(pl.multiple_of((r * n_s + s) * cs, cs), cs)].astype(F32)
        cols = lax.dot_general(
            pick, vec[...], (((1,), (1,)), ((), ())),
            precision=lax.Precision.HIGHEST, preferred_element_type=F32,
        )
        mean, scale, gain = (cols[:, base + i : base + i + 1] for i in range(3))
        spot = lax.rem(lax.broadcasted_iota(jnp.int32, (1, tall * padded), 1), padded)

        def step(f, carry):
            field = raw[layer, f].astype(F32)
            scaled = (field - mean) * scale * gain
            keep = (spot < width) & ((f >= 2) | (p > 0))
            active = jnp.where(keep, scaled * jax.nn.sigmoid(scaled), 0.0)
            act[layer, f] = active.astype(BF16)
            return carry

        lax.fori_loop(0, q * frames + 2, step, 0)

    def delta(layer, own):
        for b in range(3):
            product = None
            for f in range(q * frames):
                left = act[layer, f : f + 3].reshape(3 * cs, tall * padded)
                right = taps[layer, f, 2 - b : 2 - b + tall].reshape(tall * padded, 3 * half)
                term = jnp.dot(left, right, preferred_element_type=F32)
                product = term if product is None else product + term
            small = product.astype(BF16)
            for j in range(nj):
                for a in range(3):
                    low = a * cs + j * share
                    out[layer, j, b, a] = small[low : low + share]

                @pl.when(p == j)
                def _(j=j):
                    for a in range(3):
                        low = a * cs + j * share
                        for c in range(3):
                            own[a, b, c] = product[
                                low : low + share, c * half : (c + 1) * half
                            ]

            for k in range(1, nj):
                now = ~held | (p + k < nj) if layer == 1 and b >= SOON else None
                when(now, lambda k=k, b=b: block_copy(layer, k, b).start())

    moves_of = (moves(0, cot_ref.at[:, :, :, mine]), moves(1, gh))
    send_moves(moves_of[0], ("near", "side"))
    send_moves(moves_of[0], ("wide",))
    grads[0, own_frames, own_rows] = cot_ref[:, :, :, mine]

    field_one = f_ref[...].reshape(rows, channels).astype(F32)
    field_two = h_ref[...].reshape(rows, channels).astype(F32)
    parts = [
        jnp.sum(field_one, axis=0, keepdims=True),
        jnp.sum(field_one * field_one, axis=0, keepdims=True),
        jnp.sum(field_two, axis=0, keepdims=True),
        jnp.sum(field_two * field_two, axis=0, keepdims=True),
        jnp.zeros((4, channels), F32),
    ]
    sums_start(0, r0, jnp.concatenate(parts, axis=0))

    place_row = lax.broadcasted_iota(jnp.int32, (channels, channels), 0)
    place_col = lax.broadcasted_iota(jnp.int32, (channels, channels), 1)
    element = lax.rem(place_row, share)
    block = lax.rem(place_row // share, nj)
    which = place_row // (share * nj)
    wanted = ((block * q + which // n_s) * n_s + lax.rem(which, n_s)) * share + element
    perm[...] = jnp.where(place_col == wanted, 1.0, 0.0).astype(BF16)

    fields_two = field_moves(0)
    fields_one = field_moves(1)

    turn(h_ref, 0)
    turn(f_ref, 1)

    fill_own(0)
    conv(0, k2_ref, True)
    land(0)
    send_fields(fields_two)
    conv(0, k2_ref, False)
    gain_copy.wait()

    totals = group_sums(sums_finish(0, r0), per) / members
    mean_one, mean_two = totals[0:1], totals[2:3]
    vec[0:1] = mean_one
    vec[1:2] = lax.rsqrt(totals[1:2] - mean_one * mean_one + EPS)
    vec[2:3] = gain_ref[0:1]
    vec[3:4] = mean_two
    vec[4:5] = lax.rsqrt(totals[3:4] - mean_two * mean_two + EPS)
    vec[5:6] = gain_ref[1:2]
    vec[6:8] = jnp.zeros((2, channels), F32)

    norm_back(h_ref, 3, 0)
    for f in range(1, frames):
        send_moves(moves_of[0], (f"relay {f}",))
    send_fields(fields_one)
    gh[...] = norm_end(h_ref, 3, 0, 1).astype(BF16).reshape(frames, height, padded, half)
    send_moves(moves_of[1], ("near", "side"))
    send_moves(moves_of[1], ("wide",))
    grads[1, own_frames, own_rows] = gh[...]

    take_fields(0)
    across(0).start()
    take_moves(moves_of[0], ("wide", "relay"))
    fill_rest(0)
    across_land(0).wait_recv()
    activate(0, 3)
    delta(0, d2)
    fill_own(1)
    conv(1, k1_ref, True)
    land(1)
    conv(1, k1_ref, False)
    take_fields(1)
    across(1).start()
    norm_back(f_ref, 0, 1)
    across_land(1).wait_recv()
    activate(1, 0)
    take_moves(moves_of[1], ("wide", "relay"))
    fill_rest(1)
    delta(1, d1)
    grad = norm_end(f_ref, 0, 1, 0)
    total = cot_ref[:, :, :, mine].reshape(rows, half).astype(F32) + grad
    for f in range(frames):
        for h in range(height):
            at = (f * height + h) * padded
            mixed[f, pl.ds(h, width, stride=height)] = total[at : at + width]
    fg[...] = mixed[...].astype(BF16)
    results = [
        pltpu.make_async_copy(fg, fg_ref, o_sem.at[0]),
        pltpu.make_async_copy(weights, w_ref, o_sem.at[1]),
    ]
    for result in results:
        result.start()

    if nj > 1:
        @pl.when(held)
        def _():
            block_copy(1, 1, 0).wait_recv()
            for k in range(1, nj):
                for b in range(SOON, 3):
                    pl.when(p + k >= nj)(lambda k=k, b=b: block_copy(1, k, b).start())

    for layer, own, target in ((0, d2, d2_ref), (1, d1, d1_ref)):
        for b in range(3):
            for k in range(1, nj):
                early = layer == 1 and k == 1 and b == 0
                when(~held if early else None, lambda k=k, b=b: block_copy(layer, k, b).wait_recv())
                for a in range(3):
                    more = got[layer, k, b, a].astype(F32)
                    for c in range(3):
                        own[a, b, c] += more[:, c * half : (c + 1) * half]
            result = pltpu.make_async_copy(
                own.at[:, b], target.at[:, b], o_sem.at[2 + layer]
            )
            result.start()
        results.append(pltpu.make_async_copy(own, target, o_sem.at[2 + layer]))
    for result in results:
        result.wait()

    end_moves(moves_of[0])
    end_moves(moves_of[1])
    end_fields(0)
    end_fields(1)
    sums_end(0, r0)
    sums_end(1, r2)
    sums_end(2, r1)
    for layer in range(2):
        cross(layer).wait_send()
        across(layer).wait_send()
        for k in range(1, nj):
            whole = out.at[layer, 0]
            remote(whole, whole, dl_s.at[layer, k - 1], dl_r.at[layer, k - 1, 0], sibling).wait_send()


def hand_over(*refs):
    sources, targets, sems = refs[:4], refs[4:8], refs[8]
    copies = [
        pltpu.make_async_copy(source, target, sems.at[i])
        for i, (source, target) in enumerate(zip(sources, targets))
    ]
    for copy in copies:
        copy.start()
    for copy in copies:
        copy.wait()


def shards(n_t, n_s, features, hidden, cotangent, kernel_one, kernel_two, gains):
    frames, height, width, channels = features.shape
    half = kernel_one.shape[4]
    padded = -(-width // 16) * 16
    if padded < width + 1:
        padded += 16
    q = 2 if n_t % 2 == 0 else 1
    n = n_t * n_s
    nj = n_t // q
    share = channels // n
    cs = channels // (q * n_s)
    rows = frames * height * padded
    lanes = height * padded
    tall = n_s * height

    def wide(field):
        return jnp.pad(field, ((0, 0), (0, 0), (0, padded - width), (0, 0)))

    def stacked(kernel):
        return kernel.transpose(1, 2, 3, 0, 4).reshape(9, 3, channels, half)

    vmem = pl.BlockSpec(memory_space=pltpu.VMEM)
    hbm = pl.BlockSpec(memory_space=pltpu.HBM)
    dma = pltpu.SemaphoreType.DMA
    shapes = (
        jax.ShapeDtypeStruct((frames, height * width, half), BF16),
        jax.ShapeDtypeStruct((3, 3, 3, share, half), F32),
        jax.ShapeDtypeStruct((3, 3, 3, share, half), F32),
        jax.ShapeDtypeStruct((2, half), F32),
    )
    passed = pl.BlockSpec(memory_space=pl.ANY)
    results = pl.pallas_call(
        functools.partial(body, (width, n_t, n_s, q)),
        out_shape=shapes,
        in_specs=[vmem, vmem, vmem, hbm, hbm, hbm],
        out_specs=(passed,) * 4,
        scratch_shapes=[
            pltpu.VMEM((frames, height * width, half), BF16),
            pltpu.VMEM((frames, height * width, half), F32),
            pltpu.VMEM((3, 3, 3, share, half), F32),
            pltpu.VMEM((3, 3, 3, share, half), F32),
            pltpu.VMEM((2, half), F32),
            pltpu.VMEM((2, channels), F32),
            dma((5,)),
            pltpu.VMEM((2, q * frames + 2, tall, padded, half), BF16),
            pltpu.VMEM((2, n_s, frames, height, padded, half), BF16),
            pltpu.VMEM((2, q * frames + 2, tall + 2, padded, 3 * half), BF16),
            pltpu.VMEM((frames, height, padded, half), BF16),
            pltpu.VMEM((2, 9, channels, 3 * half), BF16),
            pltpu.VMEM((2, frames, channels, lanes), BF16),
            pltpu.VMEM((2, q * frames + 2, cs, tall * padded), BF16),
            pltpu.VMEM((2, q * frames + 2, cs, tall * padded), BF16),
            pltpu.VMEM((rows, channels), F32),
            pltpu.VMEM((2, rows, half), BF16),
            pltpu.VMEM((2, rows, half), BF16),
            pltpu.VMEM((8, channels), F32),
            pltpu.VMEM((n, 8, channels), F32),
            pltpu.VMEM((n, 8, half), F32),
            pltpu.VMEM((n, 8, half), F32),
            pltpu.VMEM((2, nj, 3, 3, share, 3 * half), BF16),
            pltpu.VMEM((2, nj, 3, 3, share, 3 * half), BF16),
            pltpu.VMEM((channels, channels), BF16),
            dma((2,)),
            dma((2, 2 * n_s - 2)), dma((2, 2, 2 * n_s - 2)),
            dma((2,)), dma((2, frames)),
            dma((2, 2)), dma((2, 2)),
            dma((2, n_s - 1)), dma((2, n_s - 1)),
            dma((2,)), dma((2, frames)),
            dma((2,)), dma((2,)),
            dma((2,)), dma((2,)),
            dma((2,)), dma((2,)),
            dma((2, nj - 1)), dma((2, nj - 1, 3)),
            dma((2,)), dma((2,)),
            dma((3,)), dma((3,)),
        ],
        compiler_params=pltpu.CompilerParams(
            collective_id=0, has_side_effects=True, vmem_limit_bytes=51 * 1024 * 1024
        ),
    )(wide(features), wide(hidden), wide(cotangent), stacked(kernel_one), stacked(kernel_two), gains)

    grad, delta_one, delta_two, weighted = pl.pallas_call(
        hand_over,
        out_shape=shapes,
        in_specs=[vmem] * 4,
        out_specs=(passed,) * 4,
        scratch_shapes=[dma((4,))],
        compiler_params=pltpu.CompilerParams(vmem_limit_bytes=8 * 1024 * 1024),
    )(*results)

    def unstacked(delta):
        return delta.transpose(3, 0, 1, 2, 4)

    feature_grad = grad.reshape(frames, width, height, half).transpose(0, 2, 1, 3)
    return (feature_grad, unstacked(delta_one), unstacked(delta_two), weighted)


def solution(mesh):
    placed = (
        P(("clip", "tm"), "space", None, None),
        P(("clip", "tm"), "space", None, None),
        P(("clip", "tm"), "space", None, None),
        P(None, None, None, None, "chan"),
        P(None, None, None, None, "chan"),
        P(),
    )
    return jax.shard_map(
        functools.partial(shards, mesh.shape["tm"], mesh.shape["space"]),
        mesh=mesh,
        in_specs=placed,
        out_specs=(
            P(("clip", "tm"), "space", None, "chan"),
            P(("clip", "tm", "space"), None, None, None, "chan"),
            P(("clip", "tm", "space"), None, None, None, "chan"),
            P("clip", "chan"),
        ),
        check_vma=False,
    )
```

```python
import functools

import jax
import jax.numpy as jnp
from jax import lax
from jax.experimental import pallas as pl
from jax.experimental.pallas import tpu as pltpu
from jax.sharding import PartitionSpec as P

GROUPS = 32
EPS = 1e-06
MESH = pl.DeviceIdType.MESH
F32 = jnp.float32
BF16 = jnp.bfloat16


def group_sums(values, per):
    channels = values.shape[1]
    row = lax.broadcasted_iota(jnp.int32, (channels, channels), 0) // per
    col = lax.broadcasted_iota(jnp.int32, (channels, channels), 1) // per
    same = jnp.where(row == col, 1.0, 0.0).astype(F32)
    return jnp.dot(values, same, precision=lax.Precision.HIGHEST, preferred_element_type=F32)


def body(
    sizes,
    f_ref, h_ref, cot_ref, k1_ref, k2_ref, gain_hbm,
    fg_ref, d1_ref, d2_ref, w_ref,
    fg, mixed, d1, d2, weights, gain_ref, o_sem,
    grads, hop, taps, gh, kcat, turned, raw, act, acc, xs, xr, vec, r0, r2, r1, out, got, perm,
    k_sem, gx_s, gx_r, gz_s, gz_r, ge_s, ge_r, gr_s, gr_r, gg_s, gg_r,
    ai_s, ai_r, an_s, an_r, ad_s, ad_r, dl_s, dl_r, xsem_s, xsem_r, ar_s, ar_r,
):
    width, n_t, n_s, q = sizes
    frames, height, padded, channels = cot_ref.shape
    half = channels // 2
    per = channels // GROUPS
    n = n_t * n_s
    nj = n_t // q
    rows = frames * height * padded
    lanes = height * padded
    tall = n_s * height
    share = channels // n
    cs = channels // (q * n_s)
    hc = cs // 2
    t = lax.axis_index("tm")
    s = lax.axis_index("space")
    chan = lax.axis_index("chan")
    partner = 1 - chan
    rank = t * n_s + s
    r = lax.rem(t, q)
    p = t // q
    held = (r == q - 1) & (p > 0)
    members = float(frames * height * width * per * n)
    mine = pl.ds(pl.multiple_of(chan * half, half), half)
    theirs = pl.ds(pl.multiple_of(partner * half, half), half)
    own_rows = pl.ds(s * height, height)
    own_frames = pl.ds(r * frames, frames)
    next_frames = pl.ds((r + 1) * frames, frames)
    sibling = {"chan": partner}

    def place(j):
        return {"tm": j // n_s, "space": lax.rem(j, n_s)}

    def peer(k):
        return lax.rem(rank + k, n)

    def each_peer(fn):
        def step(k, carry):
            fn(k)
            return carry

        lax.fori_loop(1, n, step, 0)

    def remote(src, dst, send, recv, device):
        return pltpu.make_async_remote_copy(
            src_ref=src, dst_ref=dst, send_sem=send, recv_sem=recv,
            device_id=device, device_id_type=MESH,
        )

    def kernel_copy(layer, source, c):
        return pltpu.make_async_copy(
            source.at[:, c], kcat.at[layer, :, :, c * half : (c + 1) * half], k_sem.at[layer]
        )

    for c in range(3):
        kernel_copy(0, k2_ref, c).start()
    for c in range(3):
        kernel_copy(1, k1_ref, c).start()

    gain_copy = pltpu.make_async_copy(gain_hbm, gain_ref, o_sem.at[4])
    gain_copy.start()

    barrier = pltpu.get_barrier_semaphore()
    pl.semaphore_signal(barrier, inc=1, device_id=sibling, device_id_type=MESH)
    each_peer(
        lambda k: pl.semaphore_signal(barrier, inc=1, device_id=place(peer(k)), device_id_type=MESH)
    )
    pl.semaphore_wait(barrier, n)

    def inside(value, count):
        return (value >= 0) & (value < count)

    def moves(layer, source):
        box = grads.at[layer]
        found = []
        before = jnp.where(r > 0, r, q) * frames
        sent = pl.ds(before, frames)

        def add(kind, go, src, dst, to, come, land, sender, send, recv, ends):
            found.append((
                kind, go, lambda: remote(src, dst, send, recv, to),
                come, None if land is None else lambda: remote(land, land, send, recv, sender),
                None if ends is None else lambda: remote(ends, ends, send, recv, to),
            ))

        for d, (ds, row) in enumerate(((1, height - 1), (-1, 0))):
            back = (s - ds) * height + row
            add(
                "near edge",
                (t > 0) & inside(s + ds, n_s),
                source.at[:, row : row + 1],
                box.at[sent, pl.ds(s * height + row, 1)],
                {"tm": t - 1, "space": s + ds},
                (t + 1 < n_t) & inside(s - ds, n_s),
                box.at[next_frames, pl.ds(back, 1)],
                {"tm": t + 1, "space": s - ds},
                ge_s.at[layer, d], ge_r.at[layer, d], source.at[:, row : row + 1],
            )
        for f in range(frames):
            add(
                f"near {f}", t > 0, source.at[f], box.at[before + f, own_rows], {"tm": t - 1},
                t + 1 < n_t, box.at[(r + 1) * frames + f, own_rows], {"tm": t + 1},
                gz_s.at[layer], gz_r.at[layer, f], source if f == 0 else None,
            )
        for k in sorted((k for k in range(1 - n_s, n_s) if k), key=abs):
            i = k + n_s - 1 if k < 0 else k + n_s - 2
            spans = (("wide", 0, height),)
            if abs(k) == 1:
                spans = (("near x", height - 1, 1), ("wide", 0, height - 1))
                if k < 0:
                    spans = (("near x", 0, 1), ("wide", 1, height - 1))
            for part, (kind, low, count) in enumerate(spans):
                add(
                    kind, inside(s + k, n_s), source.at[:, low : low + count],
                    box.at[own_frames, pl.ds(s * height + low, count)], {"space": s + k},
                    inside(s - k, n_s),
                    box.at[own_frames, pl.ds((s - k) * height + low, count)], {"space": s - k},
                    gx_s.at[layer, i], gx_r.at[layer, part, i], source if part == 0 else None,
                )
        if q > 1:
            for f in range(frames):
                add(
                    f"side {f}", r < q - 1,
                    source.at[f], box.at[r * frames + f, own_rows], {"tm": t + 1},
                    r > 0, box.at[(r - 1) * frames + f, own_rows], {"tm": t - 1},
                    gg_s.at[layer], gg_r.at[layer, f], source if f == 0 else None,
                )
            for k in range(1, n_s):
                to, back = lax.rem(s + k, n_s), lax.rem(s + n_s - k, n_s)
                for f in range(frames):
                    add(
                        f"relay {f}",
                        None, box.at[(q - 1 - r) * frames + f, own_rows], hop.at[layer, k, f],
                        {"space": to},
                        None, hop.at[layer, k] if f == 0 else None, {"space": back},
                        gr_s.at[layer, k - 1], gr_r.at[layer, k - 1],
                        hop.at[layer, k] if f == 0 else None,
                    )
        return found

    def when(predicate, action):
        if predicate is None:
            action()
        else:
            pl.when(predicate)(action)

    def send_moves(found, kinds):
        for kind, go, copy, *_ in found:
            if kind.startswith(kinds):
                when(go, lambda copy=copy: copy().start())

    def take_moves(found, kinds):
        for kind, _, _, come, copy, _ in found:
            if kind.startswith(kinds) and copy is not None:
                when(come, lambda copy=copy: copy().wait_recv())

    def end_moves(found):
        for _, go, _, _, _, copy in found:
            if copy is not None:
                when(go, lambda copy=copy: copy().wait_send())

    def set_rows(to_r, to_s):
        start = (to_r * n_s + to_s) * cs + chan * hc
        return pl.ds(pl.multiple_of(start, hc), hc)

    my_half = pl.ds(pl.multiple_of(chan * hc, hc), hc)

    def strip(at):
        return pl.ds(pl.multiple_of(at * lanes, lanes), lanes)

    def field_moves(layer):
        found = []
        for dr in range(q):
            for k in range(n_s):
                if dr == 0 and k == 0:
                    continue
                to_r, to_s = lax.rem(r + dr, q), lax.rem(s + k, n_s)
                src = turned.at[layer, :, set_rows(to_r, to_s)]
                dst = raw.at[layer, pl.ds(2 + r * frames, frames), my_half, strip(s)]
                found.append((None, functools.partial(
                    remote, src, dst, ai_s.at[layer], ai_r.at[layer],
                    {"tm": p * q + to_r, "space": to_s},
                )))
        for to_r in range(q):
            for k in range(n_s):
                to_s = lax.rem(s + k, n_s)
                src = turned.at[layer, frames - 2 : frames, set_rows(to_r, to_s)]
                dst = raw.at[layer, 0:2, my_half, strip(s)]
                found.append(((r == q - 1) & (p + 1 < nj), functools.partial(
                    remote, src, dst, an_s.at[layer], an_r.at[layer],
                    {"tm": (p + 1) * q + to_r, "space": to_s},
                )))
        return found

    def send_fields(found):
        for go, copy in found:
            when(go, lambda copy=copy: copy().start())

    def fields_like(layer, count, first, send, recv):
        cells = turned.at[layer, first:frames, 0 : count * hc]
        return remote(cells, cells, send.at[layer], recv.at[layer], sibling)

    def take_fields(layer):
        if q * n_s > 1:
            fields_like(layer, q * n_s - 1, 0, ai_s, ai_r).wait_recv()

        @pl.when(p > 0)
        def _():
            fields_like(layer, n_s, frames - 2, an_s, an_r).wait_recv()

    def end_fields(layer):
        if q * n_s > 1:
            fields_like(layer, q * n_s - 1, 0, ai_s, ai_r).wait_send()

        @pl.when((r == q - 1) & (p + 1 < nj))
        def _():
            fields_like(layer, q * n_s, frames - 2, an_s, an_r).wait_send()

    def across(layer):
        half_set = raw.at[layer, :, my_half]
        return remote(half_set, half_set, ad_s.at[layer], ad_r.at[layer], sibling)

    def across_land(layer):
        other = raw.at[layer, :, pl.ds(pl.multiple_of(partner * hc, hc), hc)]
        return remote(other, other, ad_s.at[layer], ad_r.at[layer], sibling)

    def sums_copy(layer, buf, device, part):
        return remote(part, part, ar_s.at[layer], ar_r.at[layer], device)

    def sums_start(layer, buf, values):
        buf[rank] = values
        each_peer(lambda k: sums_copy(layer, buf, place(peer(k)), buf.at[rank]).start())

    def sums_finish(layer, buf):
        sums_copy(layer, buf, sibling, buf.at[0 : n - 1]).wait_recv()
        return jnp.sum(buf[...], axis=0)

    def sums_end(layer, buf):
        sums_copy(layer, buf, sibling, buf.at[0 : n - 1]).wait_send()

    def block_copy(layer, k, b):
        to = lax.rem(p + k, nj)
        return remote(
            out.at[layer, to, b], got.at[layer, k, b], dl_s.at[layer, k - 1], dl_r.at[layer, k - 1, b],
            {"tm": to * q + r},
        )

    def cross(layer):
        return remote(xs.at[layer], xr.at[layer], xsem_s.at[layer], xsem_r.at[layer], sibling)

    column = lax.rem(lax.broadcasted_iota(jnp.int32, (rows, 1), 0), padded)
    real = column < width

    def spread(layer, f, row, source):
        count = source.shape[0]
        cells = source.reshape(count * padded, half).astype(F32)
        size = count * padded
        ahead = pltpu.roll(cells, size - 1, 0)
        behind = pltpu.roll(cells, 1, 0)
        for c, value in enumerate((ahead, cells, behind)):
            taps[layer, f, pl.ds(row + 1, count), :, c * half : (c + 1) * half] = value.astype(
                BF16
            ).reshape(count, padded, half)

    def fill(layer, f, row, count):
        spread(layer, f, row, grads[layer, f, pl.ds(row, count)])

    def fill_rows(layer, f):
        fill(layer, f, s * height, height)
        for row, ok in ((s * height - 1, s > 0), ((s + 1) * height, s + 1 < n_s)):
            pl.when(ok)(functools.partial(fill, layer, f, row, 1))

    def land(layer):
        take_moves(moves_of[layer], ("near edge",))
        for f in range(frames):
            take_moves(moves_of[layer], (f"near {f}", f"side {f}"))
            if layer == 1 or f == 0:
                send_moves(moves_of[layer], (f"relay {f}",))
            pl.when(t + 1 < n_t)(functools.partial(fill_rows, layer, (r + 1) * frames + f))

    def fill_own(layer):
        take_moves(moves_of[layer], ("near x",))
        for f in range(frames):
            fill_rows(layer, r * frames + f)

    def fill_rest(layer):
        for k in range(1, n_s):
            back = lax.rem(s + n_s - k, n_s)
            for f in range(frames):
                fill(layer, r * frames + f, back * height, height)
                if q > 1:
                    mate = (q - 1 - r) * frames + f
                    spread(layer, mate, back * height, hop[layer, k, f])
        if q > 1:
            @pl.when(r > 0)
            def _():
                for f in range(frames):
                    fill(layer, f, s * height, height)

    def conv(layer, source, near):
        if near:
            pltpu.make_async_copy(kcat.at[layer], kcat.at[layer], k_sem.at[layer]).wait()
        for f in range(frames):
            total = None
            for ab in range(9):
                a, b = ab // 3, ab % 3
                if (2 - a + f < frames) != near:
                    continue
                left = taps[
                    layer, r * frames + (2 - a + f), pl.ds(s * height + (2 - b), height)
                ].reshape(lanes, 3 * half)
                term = lax.dot_general(
                    left, kcat[layer, ab], (((1,), (1,)), ((), ())), preferred_element_type=F32
                )
                total = term if total is None else total + term
            if total is None:
                continue
            if near:
                acc[f * lanes : (f + 1) * lanes] = total
            else:
                acc[f * lanes : (f + 1) * lanes] += total
        if not near:
            xs[layer] = acc[:, theirs].astype(BF16)
            cross(layer).start()

    def norm_back(field_ref, base, layer):
        cross(layer).wait_recv()
        upstream = acc[:, mine] + xr[layer].astype(F32)
        field = field_ref[:, :, :, mine].reshape(rows, half).astype(F32)
        scale = vec[base + 1 : base + 2, mine]
        gain = vec[base + 2 : base + 3, mine]
        centred = (field - vec[base : base + 1, mine]) * scale
        scaled = centred * gain
        gate = jax.nn.sigmoid(scaled)
        slope = jnp.where(real, upstream * gate * (1.0 + scaled * (1.0 - gate)), 0.0)
        acc[:, mine] = slope
        parts = [
            jnp.sum(slope, axis=0, keepdims=True),
            jnp.sum(slope * centred, axis=0, keepdims=True),
            jnp.zeros((6, half), F32),
        ]
        sums_start(layer + 1, (r2, r1)[layer], jnp.concatenate(parts, axis=0))

    def norm_end(field_ref, base, layer, w_row):
        totals = sums_finish(layer + 1, (r2, r1)[layer])
        weights[w_row : w_row + 1] = totals[1:2]
        scale = vec[base + 1 : base + 2, mine]
        gain = vec[base + 2 : base + 3, mine]
        means = group_sums(totals * gain, per) / members
        field = field_ref[:, :, :, mine].reshape(rows, half).astype(F32)
        centred = (field - vec[base : base + 1, mine]) * scale
        grad = scale * (acc[:, mine] * gain - means[0:1] - centred * means[1:2])
        return jnp.where(real, grad, 0.0)

    def turn(field_ref, layer):
        for f in range(frames):
            cells = field_ref[f].reshape(lanes, channels)
            flat = lax.dot_general(
                perm[...], cells, (((1,), (1,)), ((), ())), preferred_element_type=F32
            ).astype(BF16)
            turned[layer, f] = flat
        raw[layer, pl.ds(2 + r * frames, frames), my_half, strip(s)] = turned[layer, :, set_rows(r, s)]

    def activate(layer, base):
        pick = perm[pl.ds(pl.multiple_of((r * n_s + s) * cs, cs), cs)].astype(F32)
        cols = lax.dot_general(
            pick, vec[...], (((1,), (1,)), ((), ())),
            precision=lax.Precision.HIGHEST, preferred_element_type=F32,
        )
        mean, scale, gain = (cols[:, base + i : base + i + 1] for i in range(3))
        spot = lax.rem(lax.broadcasted_iota(jnp.int32, (1, tall * padded), 1), padded)

        def step(f, carry):
            field = raw[layer, f].astype(F32)
            scaled = (field - mean) * scale * gain
            keep = (spot < width) & ((f >= 2) | (p > 0))
            active = jnp.where(keep, scaled * jax.nn.sigmoid(scaled), 0.0)
            act[layer, f] = active.astype(BF16)
            return carry

        lax.fori_loop(0, q * frames + 2, step, 0)

    def delta(layer, own):
        for b in range(3):
            product = None
            for f in range(q * frames):
                left = act[layer, f : f + 3].reshape(3 * cs, tall * padded)
                right = taps[layer, f, 2 - b : 2 - b + tall].reshape(tall * padded, 3 * half)
                term = jnp.dot(left, right, preferred_element_type=F32)
                product = term if product is None else product + term
            small = product.astype(BF16)
            for j in range(nj):
                for a in range(3):
                    low = a * cs + j * share
                    out[layer, j, b, a] = small[low : low + share]

                @pl.when(p == j)
                def _(j=j):
                    for a in range(3):
                        low = a * cs + j * share
                        for c in range(3):
                            own[a, b, c] = product[
                                low : low + share, c * half : (c + 1) * half
                            ]

            for k in range(1, nj):
                now = ~held | (p + k < nj) | (b < 2 - chan) if layer == 1 and b > 0 else None
                when(now, lambda k=k, b=b: block_copy(layer, k, b).start())

    moves_of = (moves(0, cot_ref.at[:, :, :, mine]), moves(1, gh))
    send_moves(moves_of[0], ("near", "side"))
    send_moves(moves_of[0], ("wide",))
    for layer in range(2):
        edge = jnp.zeros((q * frames + 2, 1, padded, 3 * half), BF16)
        taps[layer, :, 0:1] = edge
        taps[layer, :, tall + 1 : tall + 2] = edge

        @pl.when(t == n_t - 1)
        def _(layer=layer):
            def clear(f, carry):
                taps[layer, q * frames + f] = jnp.zeros((tall + 2, padded, 3 * half), BF16)
                return carry

            lax.fori_loop(0, 2, clear, 0)

    grads[0, own_frames, own_rows] = cot_ref[:, :, :, mine]

    field_one = f_ref[...].reshape(rows, channels).astype(F32)
    field_two = h_ref[...].reshape(rows, channels).astype(F32)
    parts = [
        jnp.sum(field_one, axis=0, keepdims=True),
        jnp.sum(field_one * field_one, axis=0, keepdims=True),
        jnp.sum(field_two, axis=0, keepdims=True),
        jnp.sum(field_two * field_two, axis=0, keepdims=True),
        jnp.zeros((4, channels), F32),
    ]
    sums_start(0, r0, jnp.concatenate(parts, axis=0))

    place_row = lax.broadcasted_iota(jnp.int32, (channels, channels), 0)
    place_col = lax.broadcasted_iota(jnp.int32, (channels, channels), 1)
    element = lax.rem(place_row, share)
    block = lax.rem(place_row // share, nj)
    which = place_row // (share * nj)
    wanted = ((block * q + which // n_s) * n_s + lax.rem(which, n_s)) * share + element
    perm[...] = jnp.where(place_col == wanted, 1.0, 0.0).astype(BF16)

    fields_two = field_moves(0)
    fields_one = field_moves(1)

    turn(h_ref, 0)
    turn(f_ref, 1)

    fill_own(0)
    conv(0, k2_ref, True)
    land(0)
    send_fields(fields_two)
    conv(0, k2_ref, False)
    gain_copy.wait()

    totals = group_sums(sums_finish(0, r0), per) / members
    mean_one, mean_two = totals[0:1], totals[2:3]
    vec[0:1] = mean_one
    vec[1:2] = lax.rsqrt(totals[1:2] - mean_one * mean_one + EPS)
    vec[2:3] = gain_ref[0:1]
    vec[3:4] = mean_two
    vec[4:5] = lax.rsqrt(totals[3:4] - mean_two * mean_two + EPS)
    vec[5:6] = gain_ref[1:2]
    vec[6:8] = jnp.zeros((2, channels), F32)

    norm_back(h_ref, 3, 0)
    for f in range(1, frames):
        send_moves(moves_of[0], (f"relay {f}",))
    send_fields(fields_one)
    gh[...] = norm_end(h_ref, 3, 0, 1).astype(BF16).reshape(frames, height, padded, half)
    send_moves(moves_of[1], ("near", "side"))
    send_moves(moves_of[1], ("wide",))
    grads[1, own_frames, own_rows] = gh[...]

    take_fields(0)
    across(0).start()
    across_land(0).wait_recv()
    activate(0, 3)
    take_moves(moves_of[0], ("wide", "relay"))
    fill_rest(0)
    delta(0, d2)
    fill_own(1)
    conv(1, k1_ref, True)
    land(1)
    conv(1, k1_ref, False)
    take_fields(1)
    across(1).start()
    norm_back(f_ref, 0, 1)
    across_land(1).wait_recv()
    activate(1, 0)
    take_moves(moves_of[1], ("wide", "relay"))
    fill_rest(1)
    delta(1, d1)
    grad = norm_end(f_ref, 0, 1, 0)
    total = cot_ref[:, :, :, mine].reshape(rows, half).astype(F32) + grad
    for f in range(frames):
        for h in range(height):
            at = (f * height + h) * padded
            mixed[f, pl.ds(h, width, stride=height)] = total[at : at + width]
    fg[...] = mixed[...].astype(BF16)
    results = [
        pltpu.make_async_copy(fg, fg_ref, o_sem.at[0]),
        pltpu.make_async_copy(weights, w_ref, o_sem.at[1]),
    ]
    for result in results:
        result.start()

    if nj > 1:
        @pl.when(held)
        def _():
            block_copy(1, 1, 0).wait_recv()
            for k in range(1, nj):
                for b in range(1, 3):
                    pl.when((p + k >= nj) & (b >= 2 - chan))(lambda k=k, b=b: block_copy(1, k, b).start())

    for layer, own, target in ((0, d2, d2_ref), (1, d1, d1_ref)):
        for b in range(3):
            for k in range(1, nj):
                early = layer == 1 and k == 1 and b == 0
                when(~held if early else None, lambda k=k, b=b: block_copy(layer, k, b).wait_recv())
                for a in range(3):
                    more = got[layer, k, b, a].astype(F32)
                    for c in range(3):
                        own[a, b, c] += more[:, c * half : (c + 1) * half]
            result = pltpu.make_async_copy(
                own.at[:, b], target.at[:, b], o_sem.at[2 + layer]
            )
            result.start()
        results.append(pltpu.make_async_copy(own, target, o_sem.at[2 + layer]))
    for result in results:
        result.wait()

    end_moves(moves_of[0])
    end_moves(moves_of[1])
    end_fields(0)
    end_fields(1)
    sums_end(0, r0)
    sums_end(1, r2)
    sums_end(2, r1)
    for layer in range(2):
        cross(layer).wait_send()
        across(layer).wait_send()
        for k in range(1, nj):
            whole = out.at[layer, 0]
            remote(whole, whole, dl_s.at[layer, k - 1], dl_r.at[layer, k - 1, 0], sibling).wait_send()


def hand_over(*refs):
    sources, targets, sems = refs[:4], refs[4:8], refs[8]
    copies = [
        pltpu.make_async_copy(source, target, sems.at[i])
        for i, (source, target) in enumerate(zip(sources, targets))
    ]
    for copy in copies:
        copy.start()
    for copy in copies:
        copy.wait()


def shards(n_t, n_s, features, hidden, cotangent, kernel_one, kernel_two, gains):
    frames, height, width, channels = features.shape
    half = kernel_one.shape[4]
    padded = -(-width // 16) * 16
    if padded < width + 1:
        padded += 16
    q = 2 if n_t % 2 == 0 else 1
    n = n_t * n_s
    nj = n_t // q
    share = channels // n
    cs = channels // (q * n_s)
    rows = frames * height * padded
    lanes = height * padded
    tall = n_s * height

    def wide(field):
        return jnp.pad(field, ((0, 0), (0, 0), (0, padded - width), (0, 0)))

    def stacked(kernel):
        return kernel.transpose(1, 2, 3, 0, 4).reshape(9, 3, channels, half)

    vmem = pl.BlockSpec(memory_space=pltpu.VMEM)
    hbm = pl.BlockSpec(memory_space=pltpu.HBM)
    dma = pltpu.SemaphoreType.DMA
    shapes = (
        jax.ShapeDtypeStruct((frames, height * width, half), BF16),
        jax.ShapeDtypeStruct((3, 3, 3, share, half), F32),
        jax.ShapeDtypeStruct((3, 3, 3, share, half), F32),
        jax.ShapeDtypeStruct((2, half), F32),
    )
    passed = pl.BlockSpec(memory_space=pl.ANY)
    results = pl.pallas_call(
        functools.partial(body, (width, n_t, n_s, q)),
        out_shape=shapes,
        in_specs=[vmem, vmem, vmem, hbm, hbm, hbm],
        out_specs=(passed,) * 4,
        scratch_shapes=[
            pltpu.VMEM((frames, height * width, half), BF16),
            pltpu.VMEM((frames, height * width, half), F32),
            pltpu.VMEM((3, 3, 3, share, half), F32),
            pltpu.VMEM((3, 3, 3, share, half), F32),
            pltpu.VMEM((2, half), F32),
            pltpu.VMEM((2, channels), F32),
            dma((5,)),
            pltpu.VMEM((2, q * frames + 2, tall, padded, half), BF16),
            pltpu.VMEM((2, n_s, frames, height, padded, half), BF16),
            pltpu.VMEM((2, q * frames + 2, tall + 2, padded, 3 * half), BF16),
            pltpu.VMEM((frames, height, padded, half), BF16),
            pltpu.VMEM((2, 9, channels, 3 * half), BF16),
            pltpu.VMEM((2, frames, channels, lanes), BF16),
            pltpu.VMEM((2, q * frames + 2, cs, tall * padded), BF16),
            pltpu.VMEM((2, q * frames + 2, cs, tall * padded), BF16),
            pltpu.VMEM((rows, channels), F32),
            pltpu.VMEM((2, rows, half), BF16),
            pltpu.VMEM((2, rows, half), BF16),
            pltpu.VMEM((8, channels), F32),
            pltpu.VMEM((n, 8, channels), F32),
            pltpu.VMEM((n, 8, half), F32),
            pltpu.VMEM((n, 8, half), F32),
            pltpu.VMEM((2, nj, 3, 3, share, 3 * half), BF16),
            pltpu.VMEM((2, nj, 3, 3, share, 3 * half), BF16),
            pltpu.VMEM((channels, channels), BF16),
            dma((2,)),
            dma((2, 2 * n_s - 2)), dma((2, 2, 2 * n_s - 2)),
            dma((2,)), dma((2, frames)),
            dma((2, 2)), dma((2, 2)),
            dma((2, n_s - 1)), dma((2, n_s - 1)),
            dma((2,)), dma((2, frames)),
            dma((2,)), dma((2,)),
            dma((2,)), dma((2,)),
            dma((2,)), dma((2,)),
            dma((2, nj - 1)), dma((2, nj - 1, 3)),
            dma((2,)), dma((2,)),
            dma((3,)), dma((3,)),
        ],
        compiler_params=pltpu.CompilerParams(
            collective_id=0, has_side_effects=True, vmem_limit_bytes=51 * 1024 * 1024
        ),
    )(wide(features), wide(hidden), wide(cotangent), stacked(kernel_one), stacked(kernel_two), gains)

    grad, delta_one, delta_two, weighted = pl.pallas_call(
        hand_over,
        out_shape=shapes,
        in_specs=[vmem] * 4,
        out_specs=(passed,) * 4,
        scratch_shapes=[dma((4,))],
        compiler_params=pltpu.CompilerParams(vmem_limit_bytes=8 * 1024 * 1024),
    )(*results)

    def unstacked(delta):
        return delta.transpose(3, 0, 1, 2, 4)

    feature_grad = grad.reshape(frames, width, height, half).transpose(0, 2, 1, 3)
    return (feature_grad, unstacked(delta_one), unstacked(delta_two), weighted)


def solution(mesh):
    placed = (
        P(("clip", "tm"), "space", None, None),
        P(("clip", "tm"), "space", None, None),
        P(("clip", "tm"), "space", None, None),
        P(None, None, None, None, "chan"),
        P(None, None, None, None, "chan"),
        P(),
    )
    return jax.shard_map(
        functools.partial(shards, mesh.shape["tm"], mesh.shape["space"]),
        mesh=mesh,
        in_specs=placed,
        out_specs=(
            P(("clip", "tm"), "space", None, "chan"),
            P(("clip", "tm", "space"), None, None, None, "chan"),
            P(("clip", "tm", "space"), None, None, None, "chan"),
            P("clip", "chan"),
        ),
        check_vma=False,
    )
```
